32 devices in a mesh: hi: 16 (over z, x, core), grp: 2 (over y).
Axes of the slice: x: 2, y: 2, z: 4, core: 2. Of those that a mesh axis runs over, the one named last changes fastest.
Arguments:
- rho: float32 [2, 8192, 8192], P(None, ('hi', 'grp')), may hold values from -6 to 9
- perm: int32 [2, 13], replicated, may hold values from 0 to 12, each once within a row
- superop: float32 [2, 2, 16, 16], replicated, may hold values from -0.3 to 1.1
Outputs:
- rho_out: float32 [2, 8192, 8192], P(None, ('hi', 'grp'))
- trace_mean: float32 [], replicated
The draws below stay inside these ranges and needn't reach their ends.
All inputs are finite; a program needn't handle non-finite values.
Results may differ from the reference program's by a relative error of at most 0.0001.
Values sent between devices are 32-bit elements; how exact they have to be, the bound alone decides.
A program may use at most 384 MiB of HBM per device.

```python
import jax
import jax.numpy as jnp
from jax import lax

QUBITS = 13
ROWS = 8192
LAYERS = 2
PAIRS = 2


def draw_rho(key, part):
    noise = jnp.clip(jax.random.normal(key, (2, ROWS, ROWS), jnp.float32), -6.0, 6.0)
    ramp = 1.0 + 2.0 * jnp.arange(ROWS, dtype=jnp.float32) / ROWS
    diagonal = jnp.eye(ROWS, dtype=jnp.float32) * ramp[None, :]
    return noise.at[0].add(diagonal)


def draw_superop(key, part):
    noise = jnp.clip(0.06 * jax.random.normal(key, (LAYERS, 2, 16, 16), jnp.float32), -0.3, 0.3)
    return noise.at[:, 0].add(0.8 * jnp.eye(16, dtype=jnp.float32)[None])


def setup_inputs(seed: int = 0) -> dict:
    seeds = jax.random.split(jax.random.key(seed), 4)
    return {
        "rho": draw_rho(jax.random.fold_in(seeds[3], 71), 0),
        "perm": jax.vmap(lambda own: jax.random.permutation(own, QUBITS))(jax.random.split(seeds[1], LAYERS)).reshape((LAYERS, QUBITS)).astype(jnp.int32),
        "superop": draw_superop(jax.random.fold_in(seeds[3], 71), 0),
    }


def relabel_table(order, count):
    positions = jnp.arange(count, dtype=jnp.int32)
    result = jnp.zeros((count,), jnp.int32)
    for qubit in range(order.shape[0]):
        bit_value = jnp.bitwise_and(jnp.right_shift(positions, qubit), 1)
        result = result + bit_value * jnp.left_shift(jnp.int32(1), order[qubit].astype(jnp.int32))
    return result


def apply_channel(matrix, layer_super, pairs):
    real_part = layer_super[0]
    imag_part = layer_super[1]
    kernel = jnp.stack([jnp.stack([real_part, -imag_part], axis=1), jnp.stack([imag_part, real_part], axis=1)], axis=0)
    kernel = kernel.reshape(2, 4, 4, 2, 4, 4)
    row_count = matrix.shape[1]
    col_count = matrix.shape[2]
    for pair_idx in range(pairs):
        inner = 4 ** pair_idx
        shaped = matrix.reshape(2, row_count // (4 * inner), 4, inner, col_count // (4 * inner), 4, inner)
        shaped = jnp.einsum("ABCrst,rhsictj->AhBicCj", kernel, shaped, precision=lax.Precision.HIGHEST)
        matrix = shaped.reshape(2, row_count, col_count)
    return matrix


def reference(rho, perm, superop):
    matrix = rho
    for layer_idx in range(LAYERS):
        index_table = relabel_table(perm[layer_idx], ROWS)
        matrix = jnp.take(matrix, index_table, axis=1)
        matrix = jnp.take(matrix, index_table, axis=2)
        matrix = apply_channel(matrix, superop[layer_idx], PAIRS)
    trace_mean = jnp.trace(matrix[0]) / ROWS
    return matrix, trace_mean
```

```python
import functools

import jax
import jax.numpy as jnp
from jax import lax
from jax.experimental import pallas as pl
from jax.experimental.pallas import tpu as pltpu
from jax.sharding import PartitionSpec as P

PAIRS = 2
SPAN = 4**PAIRS
AXES = ("hi", "grp")
VMEM_LIMIT = 60 * 1024 * 1024
LANES = 128
SIDE = 2 * SPAN * SPAN


def relabel_table(order, count):
    positions = jnp.arange(count, dtype=jnp.int32)
    result = jnp.zeros((count,), jnp.int32)
    for qubit in range(order.shape[0]):
        bit_value = jnp.bitwise_and(jnp.right_shift(positions, qubit), 1)
        result = result + bit_value * jnp.left_shift(jnp.int32(1), order[qubit])
    return result


def gather_body(idx_ref, x_ref, o_ref):
    rows = o_ref.shape[0]
    base = pl.program_id(0) * rows

    @pl.loop(0, rows // 8)
    def _(block):
        start = pl.multiple_of(block * 8, 8)
        for k in range(8):
            src = idx_ref[base + start + k]
            o_ref[pl.ds(start + k, 1), :] = x_ref[pl.ds(src, 1), :]


def gather_rows(x, idx):
    count, width = x.shape
    rows = 512
    return pl.pallas_call(
        gather_body,
        out_shape=jax.ShapeDtypeStruct(x.shape, x.dtype),
        grid_spec=pltpu.PrefetchScalarGridSpec(
            num_scalar_prefetch=1,
            grid=(count // rows,),
            in_specs=[
                pl.BlockSpec((count, width), lambda i, s: (0, 0), pipeline_mode=pl.Buffered(1))
            ],
            out_specs=pl.BlockSpec((rows, width), lambda i, s: (i, 0)),
        ),
        compiler_params=pltpu.CompilerParams(vmem_limit_bytes=VMEM_LIMIT),
        name="gather_rows",
    )(idx, x)


def gather_turn_body(idx_ref, x_ref, o_ref, tmp):
    rows = tmp.shape[0]
    low = pl.program_id(0)

    @pl.loop(0, rows // 8)
    def _(block):
        start = pl.multiple_of(block * 8, 8)
        for k in range(8):
            src = idx_ref[(start + k) * SPAN + low]
            tmp[pl.ds(start + k, 1), :] = x_ref[pl.ds(src, 1), :]

    o_ref[0] = tmp[...].T


def gather_turn(x, idx):
    count, width = x.shape
    rows = count // SPAN
    return pl.pallas_call(
        gather_turn_body,
        out_shape=jax.ShapeDtypeStruct((SPAN, width, rows), x.dtype),
        grid_spec=pltpu.PrefetchScalarGridSpec(
            num_scalar_prefetch=1,
            grid=(SPAN,),
            in_specs=[
                pl.BlockSpec((count, width), lambda i, s: (0, 0), pipeline_mode=pl.Buffered(1))
            ],
            out_specs=pl.BlockSpec((1, width, rows), lambda i, s: (i, 0, 0)),
            scratch_shapes=[pltpu.VMEM((rows, width), x.dtype)],
        ),
        compiler_params=pltpu.CompilerParams(vmem_limit_bytes=VMEM_LIMIT),
        name="gather_turn",
    )(idx, x)


def channel_body(kernel_ref, x_ref, o_ref):
    block = x_ref[...].reshape(2 * SPAN * SPAN, x_ref.shape[-1])
    mixed = jnp.dot(
        kernel_ref[...],
        block,
        precision=lax.Precision.HIGHEST,
        preferred_element_type=jnp.float32,
    )
    o_ref[...] = mixed.reshape(o_ref.shape)


def apply_channel(x, kernel):
    span, width, lanes = x.shape
    blocks = width // (2 * SPAN)
    shaped = x.reshape(span, 2, blocks, SPAN, lanes)
    side = 2 * SPAN * SPAN
    spec = pl.BlockSpec((span, 2, 1, SPAN, lanes), lambda i: (0, 0, i, 0, 0))
    whole = pl.BlockSpec((side, side), lambda i: (0, 0))
    out = pl.pallas_call(
        channel_body,
        out_shape=jax.ShapeDtypeStruct(shaped.shape, x.dtype),
        grid=(blocks,),
        in_specs=[whole, spec],
        out_specs=spec,
        compiler_params=pltpu.CompilerParams(vmem_limit_bytes=VMEM_LIMIT),
        name="channel",
    )(kernel, shaped)
    return out.reshape(x.shape)


def pair_kernel(layer_super):
    real = layer_super[0].reshape(4, 4, 4, 4)
    imag = layer_super[1].reshape(4, 4, 4, 4)

    def outer(a, b):
        both = a[:, None, :, None, :, None, :, None] * b[None, :, None, :, None, :, None, :]
        return both.reshape(SPAN, SPAN, SPAN, SPAN)

    re = outer(real, real) - outer(imag, imag)
    im = outer(real, imag) + outer(imag, real)
    top = jnp.stack([re, -im], axis=2)
    bottom = jnp.stack([im, re], axis=2)
    return jnp.stack([top, bottom], axis=0)


def exchange(x):
    return lax.all_to_all(x, AXES, split_axis=0, concat_axis=0, tiled=True)


def swap_local(x, local):
    shaped = x.reshape(x.shape[0] // local, local, 2, local)
    return jnp.transpose(shaped, (0, 3, 2, 1)).reshape(x.shape)


def simple_per_device(rho, perm, superop):
    full = rho.shape[2]
    local = rho.shape[1]
    side = 2 * SPAN * SPAN
    table0 = relabel_table(perm[0], full)
    table1 = relabel_table(perm[1], full)
    kernel0 = jnp.transpose(pair_kernel(superop[0]), (1, 0, 2, 4, 3, 5)).reshape(side, side)
    kernel1 = jnp.transpose(pair_kernel(superop[1]), (2, 0, 1, 5, 3, 4)).reshape(side, side)

    x = rho.reshape(2 * local, full).T
    x = gather_rows(x, table0)
    x = exchange(x)
    x = swap_local(x, local)
    x = gather_turn(x, table0)
    x = apply_channel(x, kernel0)
    x = jnp.transpose(x, (2, 0, 1)).reshape(full, 2 * local)
    x = gather_rows(x, table1)
    x = exchange(x)
    x = swap_local(x, local)
    x = gather_turn(x, table1)
    x = apply_channel(x, kernel1)
    x = jnp.transpose(x, (2, 0, 1)).reshape(full, 2 * local)
    matrix = x.T.reshape(2, local, full)

    return matrix


def params():
    return pltpu.CompilerParams(vmem_limit_bytes=VMEM_LIMIT)


def cost(flops, nbytes):
    return pl.CostEstimate(flops=flops, bytes_accessed=nbytes, transcendentals=0)


def whole():
    return pl.BlockSpec(memory_space=pltpu.VMEM)


def copy_rows(idx_ref, first, step, count, parts, src_ref, dst_ref, base):
    @pl.loop(0, count // 16)
    def _(block):
        start = block * 16
        for k in range(16):
            src = pl.multiple_of(idx_ref[first + step * (start + k)] * parts, parts)
            dst = pl.multiple_of((base + start + k) * parts, parts)
            dst_ref[pl.ds(dst, parts), :] = src_ref[pl.ds(src, parts), :]


def turn_body(x_ref, o_ref):
    parts = x_ref.shape[0] // LANES
    cols = x_ref.shape[1]
    for k in range(parts):
        o_ref[pl.ds(k, cols, stride=parts), :] = x_ref[pl.ds(k * LANES, LANES), :].T


def turn(x):
    height, full = x.shape
    parts = height // LANES
    cols = 512
    return pl.pallas_call(
        turn_body,
        out_shape=jax.ShapeDtypeStruct((full * parts, LANES), x.dtype),
        grid=(full // cols,),
        in_specs=[pl.BlockSpec((height, cols), lambda i: (0, i))],
        out_specs=pl.BlockSpec((cols * parts, LANES), lambda i: (i, 0)),
        compiler_params=params(),
        cost_estimate=cost(10**8, 2 * x.size * 4),
        name="turn",
    )(x)


def pick_body(chunk, local, parts, idx_ref, x_ref, o_ref):
    first = pl.program_id(0) * local + chunk * LANES
    copy_rows(idx_ref, first, 1, LANES, parts, x_ref, o_ref.at[0], 0)


def pick(xt, table, chunk, local, devices):
    parts = xt.shape[0] // (devices * local)
    return pl.pallas_call(
        functools.partial(pick_body, chunk, local, parts),
        out_shape=jax.ShapeDtypeStruct((devices, LANES * parts, LANES), xt.dtype),
        grid_spec=pltpu.PrefetchScalarGridSpec(
            num_scalar_prefetch=1,
            grid=(devices,),
            in_specs=[whole()],
            out_specs=pl.BlockSpec((1, LANES * parts, LANES), lambda i, s: (i, 0, 0)),
        ),
        compiler_params=params(),
        cost_estimate=cost(10**8, 3 * xt.size * 4),
        name="pick",
    )(table, xt)


def mix(idx_ref, w_ref, g, xk, tmp):
    high = tmp.shape[0] // 2
    groups = LANES // SPAN

    @pl.loop(0, SPAN)
    def _(low):
        copy_rows(idx_ref, low, SPAN, high, 2, g, tmp, 0)
        for part in range(2):
            turned = tmp[pl.ds(part, high, stride=2), :].T
            at = pl.multiple_of(low * 2 * SPAN + part * SPAN, SPAN)
            xk[:, pl.ds(at, SPAN), :] = turned.reshape(groups, SPAN, high)

    w = w_ref[...]
    w_big = w.astype(jnp.bfloat16)
    w_small = (w - w_big.astype(jnp.float32)).astype(jnp.bfloat16)

    @pl.loop(0, groups)
    def _(group):
        x = xk[group]
        x_big = x.astype(jnp.bfloat16)
        x_small = (x - x_big.astype(jnp.float32)).astype(jnp.bfloat16)
        y = jnp.dot(w_big, x_small, preferred_element_type=jnp.float32)
        y += jnp.dot(w_small, x_big, preferred_element_type=jnp.float32)
        y += jnp.dot(w_big, x_big, preferred_element_type=jnp.float32)
        xk[group] = y


def middle_body(local, idx_ref, next_ref, w_ref, r_ref, *refs):
    *outs, g, xk, tmp = refs
    devices = r_ref.shape[0]
    parts = r_ref.shape[1] // LANES
    halves = parts // 2
    high = tmp.shape[0] // 2

    @pl.loop(0, devices)
    def _(s):
        for k in range(parts):
            part, half = k // halves, k % halves
            block = r_ref[s, pl.ds(k, LANES, stride=parts), :]
            at = (s * local + half * LANES) * 2 + part
            g[pl.ds(at, LANES, stride=2), :] = block.T

    mix(idx_ref, w_ref, g, xk, tmp)

    @pl.loop(0, SPAN)
    def _(low):
        for part in range(2):
            at = pl.multiple_of(low * 2 * SPAN + part * SPAN, SPAN)
            block = xk[:, pl.ds(at, SPAN), :].reshape(LANES, high)
            g[pl.ds(low * high * 2 + part, high, stride=2), :] = block.T

    @pl.loop(0, devices)
    def _(d):
        for b, out in enumerate(outs):
            copy_rows(next_ref, d * local + b * LANES, 1, LANES, 2, g, out.at[d], 0)


def middle(r, table, next_table, w, local):
    devices = r.shape[0]
    full = devices * local
    high = full // SPAN
    message = jax.ShapeDtypeStruct((devices, 2 * LANES, LANES), r.dtype)
    count = local // LANES
    return pl.pallas_call(
        functools.partial(middle_body, local),
        out_shape=[message] * count,
        in_specs=[
            pl.BlockSpec(memory_space=pltpu.SMEM),
            pl.BlockSpec(memory_space=pltpu.SMEM),
            whole(),
            whole(),
        ],
        out_specs=[whole()] * count,
        scratch_shapes=[
            pltpu.VMEM((full * 2, LANES), r.dtype),
            pltpu.VMEM((LANES // SPAN, SIDE, high), r.dtype),
            pltpu.VMEM((high * 2, LANES), r.dtype),
        ],
        compiler_params=params(),
        cost_estimate=cost(2 * 3 * SIDE * full * 2 * LANES, 2 * r.size * 4),
        name="middle",
    )(table, next_table, w, r)


def last_body(local, count, idx_ref, w_ref, *refs):
    rs = refs[:count]
    o_ref, g, xk, tmp = refs[-4:]
    devices = rs[0].shape[0]
    full = devices * local
    high = tmp.shape[0] // 2
    step = pl.program_id(0)

    @pl.when(step == 0)
    def _():
        @pl.loop(0, devices)
        def _(s):
            for a, r_ref in enumerate(rs):
                for part in range(2):
                    block = r_ref[s, pl.ds(part, LANES, stride=2), :]
                    at = (s * local + a * LANES) * 2 + part
                    g[pl.ds(at, LANES, stride=2), :] = block.T

        mix(idx_ref, w_ref, g, xk, tmp)

        @pl.loop(0, SPAN)
        def _(low):
            for part in range(2):
                at = pl.multiple_of(low * 2 * SPAN + part * SPAN, SPAN)
                block = xk[:, pl.ds(at, SPAN), :].reshape(LANES, high)
                g[pl.ds(part * full + low, high, stride=SPAN), :] = block.T

    cols = o_ref.shape[2]
    for part in range(2):
        at = pl.multiple_of(part * full + step * cols, LANES)
        o_ref[part] = g[pl.ds(at, cols), :].T


def last(rs, table, w, local, which, before):
    devices = rs[0].shape[0]
    full = devices * local
    high = full // SPAN
    cols = 1024
    count = len(rs)
    extra = [] if before is None else [before]
    return pl.pallas_call(
        functools.partial(last_body, local, count),
        out_shape=jax.ShapeDtypeStruct((2, local, full), rs[0].dtype),
        grid=(full // cols,),
        in_specs=[pl.BlockSpec(memory_space=pltpu.SMEM), whole()]
        + [whole()] * count
        + [pl.BlockSpec(memory_space=pl.ANY)] * len(extra),
        out_specs=pl.BlockSpec((2, LANES, cols), lambda i: (0, which, i)),
        scratch_shapes=[
            pltpu.VMEM((full * 2, LANES), rs[0].dtype),
            pltpu.VMEM((LANES // SPAN, SIDE, high), rs[0].dtype),
            pltpu.VMEM((high * 2, LANES), rs[0].dtype),
        ],
        input_output_aliases={2 + count: 0} if extra else {},
        compiler_params=params(),
        cost_estimate=cost(2 * 3 * SIDE * full * 2 * LANES, 4 * full * 2 * LANES * 4),
        name="last",
    )(table, w, *rs, *extra)


def sum_over_devices(value, devices):
    copies = jnp.full((devices, LANES), value, value.dtype)
    return jnp.sum(exchange(copies)[:, 0])


def after(x, *done):
    return lax.optimization_barrier((x, *done))[0]


def chunked_per_device(rho, perm, superop):
    full = rho.shape[2]
    local = rho.shape[1]
    devices = full // local
    count = local // LANES
    table0 = relabel_table(perm[0], full)
    table1 = relabel_table(perm[1], full)
    spread1 = (table1 % SPAN) * (full // SPAN) + table1 // SPAN
    kernel0 = jnp.transpose(pair_kernel(superop[0]), (1, 0, 2, 4, 3, 5)).reshape(SIDE, SIDE)
    kernel1 = jnp.transpose(pair_kernel(superop[1]), (2, 0, 1, 5, 3, 4)).reshape(SIDE, SIDE)

    xt = turn(rho.reshape(2 * local, full))
    got = []
    for a in range(count):
        message = pick(xt, table0, a, local, devices)
        got.append(exchange(after(message, *got[-1:])))
    done = got[-1]
    parts = [[] for _ in range(count)]
    for a in range(count):
        messages = middle(got[a], table0, spread1, kernel0, local)
        for b, message in enumerate(messages):
            done = exchange(after(message, done))
            parts[b].append(done)
    matrix = None
    for b in range(count):
        matrix = last(parts[b], table1, kernel1, local, b, matrix)
    return matrix


def per_device(rho, perm, superop):
    full = rho.shape[2]
    local = rho.shape[1]
    run = simple_per_device if local % LANES else chunked_per_device
    matrix = run(rho, perm, superop)

    position = lax.axis_index(AXES)
    diagonal_block = lax.dynamic_slice_in_dim(matrix[0], position * local, local, 1)
    trace_total = sum_over_devices(jnp.trace(diagonal_block), full // local)
    return (matrix, trace_total / full)


def solution(mesh):
    assert PAIRS == 2
    placed = (P(None, AXES, None), P(), P())
    return jax.shard_map(
        per_device,
        mesh=mesh,
        in_specs=placed,
        out_specs=(P(None, AXES, None), P()),
        check_vma=False,
    )
```

```python
import functools

import jax
import jax.numpy as jnp
from jax import lax
from jax.experimental import pallas as pl
from jax.experimental.pallas import tpu as pltpu
from jax.sharding import PartitionSpec as P

PAIRS = 2
SPAN = 4**PAIRS
AXES = ("hi", "grp")
VMEM_LIMIT = 60 * 1024 * 1024
LANES = 128
SIDE = 2 * SPAN * SPAN
GROUPS = 2


def relabel_table(order, count):
    return relabel(jnp.arange(count, dtype=jnp.int32), order)


def relabel(positions, order):
    qubits = jnp.arange(order.shape[0], dtype=jnp.int32)[:, None]
    bits = jnp.right_shift(positions[None, :], qubits) & 1
    return jnp.sum(jnp.left_shift(bits, order[:, None]), axis=0)


def gather_body(idx_ref, x_ref, o_ref):
    rows = o_ref.shape[0]
    base = pl.program_id(0) * rows

    @pl.loop(0, rows // 8)
    def _(block):
        start = pl.multiple_of(block * 8, 8)
        for k in range(8):
            src = idx_ref[base + start + k]
            o_ref[pl.ds(start + k, 1), :] = x_ref[pl.ds(src, 1), :]


def gather_rows(x, idx):
    count, width = x.shape
    rows = 512
    return pl.pallas_call(
        gather_body,
        out_shape=jax.ShapeDtypeStruct(x.shape, x.dtype),
        grid_spec=pltpu.PrefetchScalarGridSpec(
            num_scalar_prefetch=1,
            grid=(count // rows,),
            in_specs=[
                pl.BlockSpec((count, width), lambda i, s: (0, 0), pipeline_mode=pl.Buffered(1))
            ],
            out_specs=pl.BlockSpec((rows, width), lambda i, s: (i, 0)),
        ),
        compiler_params=pltpu.CompilerParams(vmem_limit_bytes=VMEM_LIMIT),
        name="gather_rows",
    )(idx, x)


def gather_turn_body(idx_ref, x_ref, o_ref, tmp):
    rows = tmp.shape[0]
    low = pl.program_id(0)

    @pl.loop(0, rows // 8)
    def _(block):
        start = pl.multiple_of(block * 8, 8)
        for k in range(8):
            src = idx_ref[(start + k) * SPAN + low]
            tmp[pl.ds(start + k, 1), :] = x_ref[pl.ds(src, 1), :]

    o_ref[0] = tmp[...].T


def gather_turn(x, idx):
    count, width = x.shape
    rows = count // SPAN
    return pl.pallas_call(
        gather_turn_body,
        out_shape=jax.ShapeDtypeStruct((SPAN, width, rows), x.dtype),
        grid_spec=pltpu.PrefetchScalarGridSpec(
            num_scalar_prefetch=1,
            grid=(SPAN,),
            in_specs=[
                pl.BlockSpec((count, width), lambda i, s: (0, 0), pipeline_mode=pl.Buffered(1))
            ],
            out_specs=pl.BlockSpec((1, width, rows), lambda i, s: (i, 0, 0)),
            scratch_shapes=[pltpu.VMEM((rows, width), x.dtype)],
        ),
        compiler_params=pltpu.CompilerParams(vmem_limit_bytes=VMEM_LIMIT),
        name="gather_turn",
    )(idx, x)


def channel_body(kernel_ref, x_ref, o_ref):
    block = x_ref[...].reshape(2 * SPAN * SPAN, x_ref.shape[-1])
    mixed = jnp.dot(
        kernel_ref[...],
        block,
        precision=lax.Precision.HIGHEST,
        preferred_element_type=jnp.float32,
    )
    o_ref[...] = mixed.reshape(o_ref.shape)


def apply_channel(x, kernel):
    span, width, lanes = x.shape
    blocks = width // (2 * SPAN)
    shaped = x.reshape(span, 2, blocks, SPAN, lanes)
    side = 2 * SPAN * SPAN
    spec = pl.BlockSpec((span, 2, 1, SPAN, lanes), lambda i: (0, 0, i, 0, 0))
    whole = pl.BlockSpec((side, side), lambda i: (0, 0))
    out = pl.pallas_call(
        channel_body,
        out_shape=jax.ShapeDtypeStruct(shaped.shape, x.dtype),
        grid=(blocks,),
        in_specs=[whole, spec],
        out_specs=spec,
        compiler_params=pltpu.CompilerParams(vmem_limit_bytes=VMEM_LIMIT),
        name="channel",
    )(kernel, shaped)
    return out.reshape(x.shape)


def pair_kernel(layer_super):
    real = layer_super[0].reshape(4, 4, 4, 4)
    imag = layer_super[1].reshape(4, 4, 4, 4)

    def outer(a, b):
        both = a[:, None, :, None, :, None, :, None] * b[None, :, None, :, None, :, None, :]
        return both.reshape(SPAN, SPAN, SPAN, SPAN)

    re = outer(real, real) - outer(imag, imag)
    im = outer(real, imag) + outer(imag, real)
    top = jnp.stack([re, -im], axis=2)
    bottom = jnp.stack([im, re], axis=2)
    return jnp.stack([top, bottom], axis=0)


def exchange(x, groups=None):
    return lax.all_to_all(
        x, AXES, split_axis=0, concat_axis=0, tiled=True, axis_index_groups=groups
    )


def swap_local(x, local):
    shaped = x.reshape(x.shape[0] // local, local, 2, local)
    return jnp.transpose(shaped, (0, 3, 2, 1)).reshape(x.shape)


def simple_per_device(rho, perm, superop):
    full = rho.shape[2]
    local = rho.shape[1]
    side = 2 * SPAN * SPAN
    table0 = relabel_table(perm[0], full)
    table1 = relabel_table(perm[1], full)
    kernel0 = jnp.transpose(pair_kernel(superop[0]), (1, 0, 2, 4, 3, 5)).reshape(side, side)
    kernel1 = jnp.transpose(pair_kernel(superop[1]), (2, 0, 1, 5, 3, 4)).reshape(side, side)

    x = rho.reshape(2 * local, full).T
    x = gather_rows(x, table0)
    x = exchange(x)
    x = swap_local(x, local)
    x = gather_turn(x, table0)
    x = apply_channel(x, kernel0)
    x = jnp.transpose(x, (2, 0, 1)).reshape(full, 2 * local)
    x = gather_rows(x, table1)
    x = exchange(x)
    x = swap_local(x, local)
    x = gather_turn(x, table1)
    x = apply_channel(x, kernel1)
    x = jnp.transpose(x, (2, 0, 1)).reshape(full, 2 * local)
    matrix = x.T.reshape(2, local, full)

    return matrix


def params():
    return pltpu.CompilerParams(vmem_limit_bytes=VMEM_LIMIT)


def cost(flops, nbytes):
    return pl.CostEstimate(flops=flops, bytes_accessed=nbytes, transcendentals=0)


def whole():
    return pl.BlockSpec(memory_space=pltpu.VMEM)


def scalars():
    return pl.BlockSpec(memory_space=pltpu.SMEM)


def two_parts(x):
    big = x.astype(jnp.bfloat16)
    return big, (x - big.astype(jnp.float32)).astype(jnp.bfloat16)


def reorder(order, x):
    big, small = two_parts(x)
    y = jnp.dot(order, small, preferred_element_type=jnp.float32)
    return y + jnp.dot(order, big, preferred_element_type=jnp.float32)


def copy_rows(idx_ref, first, step, count, parts, src_ref, dst_ref, base, whole_row=None, skip=0):
    pitch = parts if whole_row is None else whole_row

    @pl.loop(0, count // 16)
    def _(block):
        start = block * 16
        for k in range(16):
            src = pl.multiple_of(idx_ref[first + step * (start + k)] * pitch + skip, parts)
            dst = pl.multiple_of((base + start + k) * parts, parts)
            dst_ref[pl.ds(dst, parts), :] = src_ref[pl.ds(src, parts), :]


def superop_body(by_row, s_ref, o_ref):
    at = lax.broadcasted_iota(jnp.int32, (SIDE, SPAN), 0)
    entry = lax.broadcasted_iota(jnp.int32, (SIDE, SPAN), 1)
    first, last_ = at // (2 * SPAN), at % SPAN
    row, col = (first, last_) if by_row else (last_, first)

    def spread(pair, values):
        mine = jnp.right_shift(row, 2 * pair) % 4 * 4 + jnp.right_shift(col, 2 * pair) % 4
        pick_ = jnp.where(mine == entry, 1.0, 0.0)
        rows = jnp.dot(
            pick_, values, precision=lax.Precision.HIGHEST, preferred_element_type=jnp.float32
        )
        return lax.dot_general(
            rows,
            pick_,
            (((1,), (1,)), ((), ())),
            precision=lax.Precision.HIGHEST,
            preferred_element_type=jnp.float32,
        )

    re0, im0 = spread(0, s_ref[0]), spread(0, s_ref[1])
    re1, im1 = spread(1, s_ref[0]), spread(1, s_ref[1])
    re = re1 * re0 - im1 * im0
    im = re1 * im0 + im1 * re0
    out_im = lax.broadcasted_iota(jnp.int32, (SIDE, SIDE), 0) // SPAN % 2
    in_im = lax.broadcasted_iota(jnp.int32, (SIDE, SIDE), 1) // SPAN % 2
    o_ref[...] = jnp.where(out_im == in_im, re, jnp.where(out_im == 1, im, -im))


def superop_matrix(layer_super, by_row):
    return pl.pallas_call(
        functools.partial(superop_body, by_row),
        out_shape=jax.ShapeDtypeStruct((SIDE, SIDE), jnp.float32),
        in_specs=[whole()],
        out_specs=whole(),
        compiler_params=params(),
        cost_estimate=cost(10**8, 10**6),
        name="superop",
    )(layer_super)


def turn_body(x_ref, o_ref):
    parts = x_ref.shape[0] // LANES
    cols = x_ref.shape[1]
    for k in range(parts):
        o_ref[pl.ds(k, cols, stride=parts), :] = x_ref[pl.ds(k * LANES, LANES), :].T


def turn_order_body(order_ref, x_ref, o_ref):
    parts = x_ref.shape[0] // LANES
    cols = x_ref.shape[1]
    half = parts // 2
    order = order_ref[...].astype(jnp.bfloat16)
    for part in range(2):
        x = reorder(order, x_ref[pl.ds(part * half * LANES, half * LANES), :])
        for k in range(half):
            o_ref[pl.ds(k * 2 + part, cols, stride=parts), :] = x[k * LANES : (k + 1) * LANES].T


def turn(x, order=None):
    height, full = x.shape
    parts = height // LANES
    cols = 512
    extra = [] if order is None else [order]
    return pl.pallas_call(
        turn_body if order is None else turn_order_body,
        out_shape=jax.ShapeDtypeStruct((full * parts, LANES), x.dtype),
        grid=(full // cols,),
        in_specs=[pl.BlockSpec(o.shape, lambda i: (0, 0)) for o in extra]
        + [pl.BlockSpec((height, cols), lambda i: (0, i))],
        out_specs=pl.BlockSpec((cols * parts, LANES), lambda i: (i, 0)),
        compiler_params=params(),
        cost_estimate=cost(10**8, 2 * x.size * 4),
        name="turn",
    )(*extra, x)


def pick_body(group, share, devices, parts, idx_ref, x_ref, o_ref):
    count = share // GROUPS
    targets = o_ref.shape[0]
    senders = x_ref.shape[0] // (parts * idx_ref.shape[0])

    @pl.loop(0, targets)
    def _(i):
        d = pl.program_id(0) * targets + i
        first = d % devices * share + group * count
        skip = d // devices * parts
        copy_rows(idx_ref, first, 1, count, parts, x_ref, o_ref.at[i], 0, senders * parts, skip)


def pick(xt, table, group, devices, parts):
    full = table.shape[0]
    share = full // devices
    targets = devices * (xt.shape[0] // (full * parts))
    steps = 4
    rows = share // GROUPS * parts
    return pl.pallas_call(
        functools.partial(pick_body, group, share, devices, parts),
        out_shape=jax.ShapeDtypeStruct((targets, rows, LANES), xt.dtype),
        grid_spec=pltpu.PrefetchScalarGridSpec(
            num_scalar_prefetch=1,
            grid=(steps,),
            in_specs=[whole()],
            out_specs=pl.BlockSpec((targets // steps, rows, LANES), lambda i, s: (i, 0, 0)),
        ),
        compiler_params=params(),
        cost_estimate=cost(10**8, 3 * xt.size * 4),
        name="pick",
    )(table, xt)


def mix(idx_ref, w_ref, g, xk, tmp):
    high = tmp.shape[0] // 2
    groups = LANES // SPAN

    @pl.loop(0, SPAN)
    def _(low):
        copy_rows(idx_ref, low, SPAN, high, 2, g, tmp, 0)
        for part in range(2):
            turned = tmp[pl.ds(part, high, stride=2), :].T
            at = pl.multiple_of(low * 2 * SPAN + part * SPAN, SPAN)
            xk[:, pl.ds(at, SPAN), :] = turned.reshape(groups, SPAN, high)

    w_big, w_small = two_parts(w_ref[...])

    @pl.loop(0, groups)
    def _(group):
        x_big, x_small = two_parts(xk[group])
        y = jnp.dot(w_big, x_small, preferred_element_type=jnp.float32)
        y += jnp.dot(w_small, x_big, preferred_element_type=jnp.float32)
        y += jnp.dot(w_big, x_big, preferred_element_type=jnp.float32)
        xk[group] = y


def middle_body(chunks, count, blocks, idx_ref, next_ref, w_ref, r_ref, *refs):
    *outs, g, xk, tmp = refs
    sources = r_ref.shape[0]
    parts = r_ref.shape[1] // (LANES * chunks)
    halves = parts // 2
    local = halves * LANES
    high = tmp.shape[0] // 2
    rows = next_ref.shape[0] // (outs[0].shape[0] * blocks)

    @pl.loop(0, chunks)
    def _(c):
        @pl.loop(0, sources)
        def _(s):
            for k in range(parts):
                part, half = k // halves, k % halves
                block = r_ref[s, pl.ds(c * (LANES * parts) + k, LANES, stride=parts), :]
                at = (s * local + half * LANES) * 2 + part
                g[pl.ds(at, LANES, stride=2), :] = block.T

        mix(idx_ref, w_ref, g, xk, tmp)

        @pl.loop(0, SPAN)
        def _(low):
            for part in range(2):
                at = pl.multiple_of(low * 2 * SPAN + part * SPAN, SPAN)
                block = xk[:, pl.ds(at, SPAN), :].reshape(LANES, high)
                g[pl.ds(low * high * 2 + part, high, stride=2), :] = block.T

        @pl.loop(0, outs[0].shape[0])
        def _(d):
            for b in range(blocks):
                out, base = (outs[0], (c * blocks + b) * rows) if count == 1 else (outs[b], c * rows)
                copy_rows(next_ref, (d * blocks + b) * rows, 1, rows, 2, g, out.at[d], base)


def middle(r, table, next_table, w, chunks, devices, blocks, split):
    full = table.shape[0]
    high = full // SPAN
    count = blocks if split else 1
    rows = next_table.shape[0] // (devices * blocks) * chunks * (blocks // count)
    message = jax.ShapeDtypeStruct((devices, 2 * rows, LANES), r.dtype)
    return pl.pallas_call(
        functools.partial(middle_body, chunks, count, blocks),
        out_shape=[message] * count,
        in_specs=[scalars(), scalars(), whole(), whole()],
        out_specs=[whole()] * count,
        scratch_shapes=[
            pltpu.VMEM((full * 2, LANES), r.dtype),
            pltpu.VMEM((LANES // SPAN, SIDE, high), r.dtype),
            pltpu.VMEM((high * 2, LANES), r.dtype),
        ],
        compiler_params=params(),
        cost_estimate=cost(2 * 3 * SIDE * r.size, 2 * r.size * 4),
        name="middle",
    )(table, next_table, w, r)


def last_body(chunks, which, blocks, paired, idx_ref, w_ref, *refs):
    if paired:
        order_ref, *refs = refs
    rs = refs[:GROUPS]
    o_ref, g, xk, tmp = refs[-4:]
    full = idx_ref.shape[0]
    high = tmp.shape[0] // 2
    step = pl.program_id(0)
    sources = rs[0].shape[0] // (2 if paired else 1)
    rows = LANES // (2 if paired else 1)
    share = full // sources

    @pl.when(step == 0)
    def _():
        if paired:
            order = order_ref[...].astype(jnp.bfloat16)

        @pl.loop(0, sources)
        def _(s):
            for a, r_ref in enumerate(rs):
                there = blocks if r_ref.shape[1] == 2 * rows * chunks * blocks else 1
                for c in range(chunks):
                    for part in range(2):
                        base = (c * there + (which if there > 1 else 0)) * rows * 2 + part
                        at = pl.ds(base, rows, stride=2)
                        if paired:
                            block = jnp.concatenate([r_ref[s, at, :], r_ref[s + sources, at, :]])
                            block = reorder(order, block)
                        else:
                            block = r_ref[s, at, :]
                        to = (s * share + (a * chunks + c) * LANES) * 2 + part
                        g[pl.ds(to, LANES, stride=2), :] = block.T

        mix(idx_ref, w_ref, g, xk, tmp)

        @pl.loop(0, SPAN)
        def _(low):
            for part in range(2):
                at = pl.multiple_of(low * 2 * SPAN + part * SPAN, SPAN)
                block = xk[:, pl.ds(at, SPAN), :].reshape(LANES, high)
                g[pl.ds(part * full + low, high, stride=SPAN), :] = block.T

    cols = o_ref.shape[2]
    for part in range(2):
        at = pl.multiple_of(part * full + step * cols, LANES)
        o_ref[part] = g[pl.ds(at, cols), :].T


def last(rs, table, w, order, chunks, which, blocks, before):
    full = table.shape[0]
    high = full // SPAN
    cols = 1024
    orders = [] if order is None else [order]
    extra = [] if before is None else [before]
    ins = [table, w, *orders, *rs]
    return pl.pallas_call(
        functools.partial(last_body, chunks, which, blocks, order is not None),
        out_shape=jax.ShapeDtypeStruct((2, blocks * LANES, full), rs[0].dtype),
        grid=(full // cols,),
        in_specs=[scalars()]
        + [whole()] * (len(ins) - 1)
        + [pl.BlockSpec(memory_space=pl.ANY)] * len(extra),
        out_specs=pl.BlockSpec((2, LANES, cols), lambda i: (0, which, i)),
        scratch_shapes=[
            pltpu.VMEM((full * 2, LANES), rs[0].dtype),
            pltpu.VMEM((LANES // SPAN, SIDE, high), rs[0].dtype),
            pltpu.VMEM((high * 2, LANES), rs[0].dtype),
        ],
        input_output_aliases={len(ins): 0} if extra else {},
        compiler_params=params(),
        cost_estimate=cost(2 * 3 * SIDE * full * 2 * LANES, 4 * full * 2 * LANES * 4),
        name="last",
    )(*ins, *extra)


def sum_over_devices(value, devices):
    copies = jnp.full((devices, LANES), value, value.dtype)
    return jnp.sum(exchange(copies)[:, 0])


def after(x, *done):
    return lax.optimization_barrier((x, *done))[0]


def bit_in(x, at):
    low = jnp.left_shift(1, at) - 1
    return jnp.left_shift(x - (x & low), 1) + (x & low)


def bit_out(x, at):
    low = jnp.left_shift(1, at) - 1
    return jnp.left_shift(jnp.right_shift(x, at + 1), at) + (x & low)


def spread(q, count):
    return q % SPAN * (count // SPAN) + q // SPAN


def run_plan(plan, rho, perm, superop, devices):
    full = rho.shape[2]
    local = full // devices
    blocks = local // LANES
    top = full // 2
    half = devices // 2
    halves = [list(range(half)), list(range(half, devices))]
    top_bit = top.bit_length() - 1
    table0 = relabel_table(perm[0], full)
    kept = jnp.argmax(perm[0] == top_bit).astype(jnp.int32)
    final = perm[1][top_bit]
    x = rho.reshape(2 * local, full)
    q = jnp.arange(top, dtype=jnp.int32)
    first_groups = second_groups = order = None

    if plan == "full":
        share, parts, chunks = devices, 2 * blocks, 1
        xt = turn(x)
        rows0 = table0
        rows1 = spread(relabel_table(perm[1], full), full)
        targets = devices
    else:
        share, chunks = half, 2
        if plan == "send_keep":
            parts = 2
            source = perm[0][final]
            at = jnp.arange(local, dtype=jnp.int32)
            new = bit_out(at, source) + (jnp.right_shift(at, source) & 1) * (local // 2)
            xt = turn(x, jnp.where(at[:, None] == new[None, :], 1.0, 0.0))
            old = relabel(bit_in(q, final), perm[0])
            rows0 = old // local * (local // 2) + bit_out(old % local, source)
            stays = final
        else:
            parts = 2 * blocks
            first_groups = halves
            xt = turn(x)
            rows0 = relabel(bit_in(q, kept), perm[0])
            stays = kept
        if plan == "keep_send":
            targets = devices
            place = jnp.argmax(perm[1] == kept).astype(jnp.int32)
            few = LANES // 2
            row = q // few * LANES + bit_in(q % few, place)
            at = jnp.arange(LANES, dtype=jnp.int32)
            sent = bit_in(at % few, place) + jnp.left_shift(at // few, place)
            order = jnp.where(at[:, None] == sent[None, :], 1.0, 0.0)
        else:
            targets = half
            second_groups = halves
            row = q
        rows1 = spread(bit_out(relabel(row, perm[1]), stays), top)

    table1 = relabel_table(perm[1], full)
    got = []
    for a in range(GROUPS):
        message = pick(xt, table0, a, share, parts)
        got.append(exchange(after(message, *got[-1:]), first_groups))
    kernel0 = superop_matrix(superop[0], True)
    kernel1 = superop_matrix(superop[1], False)
    done = got[-1]
    parts_of = [[] for _ in range(blocks)]
    for a in range(GROUPS):
        split = a == GROUPS - 1
        messages = middle(got[a], rows0, rows1, kernel0, chunks, targets, blocks, split)
        arrived = []
        for message in messages:
            done = exchange(after(message, done), second_groups)
            arrived.append(done)
        for b in range(blocks):
            parts_of[b].append(arrived[b] if split else arrived[0])
    matrix = None
    for b in range(blocks):
        matrix = last(parts_of[b], table1, kernel1, order, chunks, b, blocks, matrix)
    return matrix


def choose_plan(perm, devices, local):
    top_bit = perm.shape[1] - 1
    low_bits = (SPAN - 1).bit_length()
    kept = jnp.argmax(perm[0] == top_bit).astype(jnp.int32)
    place = jnp.argmax(perm[1] == kept).astype(jnp.int32)
    final = perm[1][top_bit]
    source = perm[0][final]
    plain = kept >= low_bits
    keep_send = plain & (place < LANES.bit_length() - 1)
    keep_keep = plain & (place == top_bit)
    send_keep = (kept < low_bits) & (final >= low_bits) & (source < local.bit_length() - 1)
    return jnp.where(keep_send, 1, jnp.where(keep_keep, 2, jnp.where(send_keep, 3, 0)))


def chunked_per_device(rho, perm, superop):
    full = rho.shape[2]
    local = rho.shape[1]
    devices = full // local
    plans = ("full", "keep_send", "keep_keep", "send_keep")
    runs = [functools.partial(run_plan, plan, devices=devices) for plan in plans]
    return lax.switch(choose_plan(perm, devices, local), runs, rho, perm, superop)


def per_device(rho, perm, superop):
    full = rho.shape[2]
    local = rho.shape[1]
    run = chunked_per_device if local == GROUPS * LANES else simple_per_device
    matrix = run(rho, perm, superop)

    position = lax.axis_index(AXES)
    diagonal_block = lax.dynamic_slice_in_dim(matrix[0], position * local, local, 1)
    trace_total = sum_over_devices(jnp.trace(diagonal_block), full // local)
    return (matrix, trace_total / full)


def solution(mesh):
    assert PAIRS == 2
    placed = (P(None, AXES, None), P(), P())
    return jax.shard_map(
        per_device,
        mesh=mesh,
        in_specs=placed,
        out_specs=(P(None, AXES, None), P()),
        check_vma=False,
    )
```

```python
import functools

import jax
import jax.numpy as jnp
from jax import lax
from jax.experimental import pallas as pl
from jax.experimental.pallas import tpu as pltpu
from jax.sharding import PartitionSpec as P

PAIRS = 2
SPAN = 4**PAIRS
AXES = ("hi", "grp")
VMEM_LIMIT = 60 * 1024 * 1024
LANES = 128
SIDE = 2 * SPAN * SPAN
GROUPS = 2


def relabel_table(order, count):
    return relabel(jnp.arange(count, dtype=jnp.int32), order)


def relabel(positions, order):
    qubits = jnp.arange(order.shape[0], dtype=jnp.int32)[:, None]
    bits = jnp.right_shift(positions[None, :], qubits) & 1
    return jnp.sum(jnp.left_shift(bits, order[:, None]), axis=0)


def gather_body(idx_ref, x_ref, o_ref):
    rows = o_ref.shape[0]
    base = pl.program_id(0) * rows

    @pl.loop(0, rows // 8)
    def _(block):
        start = pl.multiple_of(block * 8, 8)
        for k in range(8):
            src = idx_ref[base + start + k]
            o_ref[pl.ds(start + k, 1), :] = x_ref[pl.ds(src, 1), :]


def gather_rows(x, idx):
    count, width = x.shape
    rows = 512
    return pl.pallas_call(
        gather_body,
        out_shape=jax.ShapeDtypeStruct(x.shape, x.dtype),
        grid_spec=pltpu.PrefetchScalarGridSpec(
            num_scalar_prefetch=1,
            grid=(count // rows,),
            in_specs=[
                pl.BlockSpec((count, width), lambda i, s: (0, 0), pipeline_mode=pl.Buffered(1))
            ],
            out_specs=pl.BlockSpec((rows, width), lambda i, s: (i, 0)),
        ),
        compiler_params=pltpu.CompilerParams(vmem_limit_bytes=VMEM_LIMIT),
        name="gather_rows",
    )(idx, x)


def gather_turn_body(idx_ref, x_ref, o_ref, tmp):
    rows = tmp.shape[0]
    low = pl.program_id(0)

    @pl.loop(0, rows // 8)
    def _(block):
        start = pl.multiple_of(block * 8, 8)
        for k in range(8):
            src = idx_ref[(start + k) * SPAN + low]
            tmp[pl.ds(start + k, 1), :] = x_ref[pl.ds(src, 1), :]

    o_ref[0] = tmp[...].T


def gather_turn(x, idx):
    count, width = x.shape
    rows = count // SPAN
    return pl.pallas_call(
        gather_turn_body,
        out_shape=jax.ShapeDtypeStruct((SPAN, width, rows), x.dtype),
        grid_spec=pltpu.PrefetchScalarGridSpec(
            num_scalar_prefetch=1,
            grid=(SPAN,),
            in_specs=[
                pl.BlockSpec((count, width), lambda i, s: (0, 0), pipeline_mode=pl.Buffered(1))
            ],
            out_specs=pl.BlockSpec((1, width, rows), lambda i, s: (i, 0, 0)),
            scratch_shapes=[pltpu.VMEM((rows, width), x.dtype)],
        ),
        compiler_params=pltpu.CompilerParams(vmem_limit_bytes=VMEM_LIMIT),
        name="gather_turn",
    )(idx, x)


def channel_body(kernel_ref, x_ref, o_ref):
    block = x_ref[...].reshape(2 * SPAN * SPAN, x_ref.shape[-1])
    mixed = jnp.dot(
        kernel_ref[...],
        block,
        precision=lax.Precision.HIGHEST,
        preferred_element_type=jnp.float32,
    )
    o_ref[...] = mixed.reshape(o_ref.shape)


def apply_channel(x, kernel):
    span, width, lanes = x.shape
    blocks = width // (2 * SPAN)
    shaped = x.reshape(span, 2, blocks, SPAN, lanes)
    side = 2 * SPAN * SPAN
    spec = pl.BlockSpec((span, 2, 1, SPAN, lanes), lambda i: (0, 0, i, 0, 0))
    whole = pl.BlockSpec((side, side), lambda i: (0, 0))
    out = pl.pallas_call(
        channel_body,
        out_shape=jax.ShapeDtypeStruct(shaped.shape, x.dtype),
        grid=(blocks,),
        in_specs=[whole, spec],
        out_specs=spec,
        compiler_params=pltpu.CompilerParams(vmem_limit_bytes=VMEM_LIMIT),
        name="channel",
    )(kernel, shaped)
    return out.reshape(x.shape)


def pair_kernel(layer_super):
    real = layer_super[0].reshape(4, 4, 4, 4)
    imag = layer_super[1].reshape(4, 4, 4, 4)

    def outer(a, b):
        both = a[:, None, :, None, :, None, :, None] * b[None, :, None, :, None, :, None, :]
        return both.reshape(SPAN, SPAN, SPAN, SPAN)

    re = outer(real, real) - outer(imag, imag)
    im = outer(real, imag) + outer(imag, real)
    top = jnp.stack([re, -im], axis=2)
    bottom = jnp.stack([im, re], axis=2)
    return jnp.stack([top, bottom], axis=0)


def exchange(x, groups=None):
    return lax.all_to_all(
        x, AXES, split_axis=0, concat_axis=0, tiled=True, axis_index_groups=groups
    )


def swap_local(x, local):
    shaped = x.reshape(x.shape[0] // local, local, 2, local)
    return jnp.transpose(shaped, (0, 3, 2, 1)).reshape(x.shape)


def simple_per_device(rho, perm, superop):
    full = rho.shape[2]
    local = rho.shape[1]
    side = 2 * SPAN * SPAN
    table0 = relabel_table(perm[0], full)
    table1 = relabel_table(perm[1], full)
    kernel0 = jnp.transpose(pair_kernel(superop[0]), (1, 0, 2, 4, 3, 5)).reshape(side, side)
    kernel1 = jnp.transpose(pair_kernel(superop[1]), (2, 0, 1, 5, 3, 4)).reshape(side, side)

    x = rho.reshape(2 * local, full).T
    x = gather_rows(x, table0)
    x = exchange(x)
    x = swap_local(x, local)
    x = gather_turn(x, table0)
    x = apply_channel(x, kernel0)
    x = jnp.transpose(x, (2, 0, 1)).reshape(full, 2 * local)
    x = gather_rows(x, table1)
    x = exchange(x)
    x = swap_local(x, local)
    x = gather_turn(x, table1)
    x = apply_channel(x, kernel1)
    x = jnp.transpose(x, (2, 0, 1)).reshape(full, 2 * local)
    matrix = x.T.reshape(2, local, full)

    return matrix


def params():
    return pltpu.CompilerParams(vmem_limit_bytes=VMEM_LIMIT)


def cost(flops, nbytes):
    return pl.CostEstimate(flops=flops, bytes_accessed=nbytes, transcendentals=0)


def whole():
    return pl.BlockSpec(memory_space=pltpu.VMEM)


def scalars():
    return pl.BlockSpec(memory_space=pltpu.SMEM)


def two_parts(x):
    big = x.astype(jnp.bfloat16)
    return big, (x - big.astype(jnp.float32)).astype(jnp.bfloat16)


def reorder(order, x):
    big, small = two_parts(x)
    y = jnp.dot(order, small, preferred_element_type=jnp.float32)
    return y + jnp.dot(order, big, preferred_element_type=jnp.float32)


def copy_rows(idx_ref, first, step, count, parts, src_ref, dst_ref, base, whole_row=None, skip=0):
    pitch = parts if whole_row is None else whole_row
    near = [idx_ref[step * k] * pitch for k in range(8)]

    @pl.loop(0, count // 16)
    def _(block):
        start = block * 16
        for far in range(0, 16, 8):
            origin = idx_ref[first + step * (start + far)] * pitch + skip
            for k in range(8):
                src = pl.multiple_of(origin + near[k], parts)
                dst = pl.multiple_of((base + start + far + k) * parts, parts)
                dst_ref[pl.ds(dst, parts), :] = src_ref[pl.ds(src, parts), :]


def superop_body(by_row, s_ref, o_ref):
    at = lax.broadcasted_iota(jnp.int32, (SIDE, SPAN), 0)
    entry = lax.broadcasted_iota(jnp.int32, (SIDE, SPAN), 1)
    first, last_ = at // (2 * SPAN), at % SPAN
    row, col = (first, last_) if by_row else (last_, first)

    def spread(pair, values):
        mine = jnp.right_shift(row, 2 * pair) % 4 * 4 + jnp.right_shift(col, 2 * pair) % 4
        pick_ = jnp.where(mine == entry, 1.0, 0.0)
        rows = jnp.dot(
            pick_, values, precision=lax.Precision.HIGHEST, preferred_element_type=jnp.float32
        )
        return lax.dot_general(
            rows,
            pick_,
            (((1,), (1,)), ((), ())),
            precision=lax.Precision.HIGHEST,
            preferred_element_type=jnp.float32,
        )

    re0, im0 = spread(0, s_ref[0]), spread(0, s_ref[1])
    re1, im1 = spread(1, s_ref[0]), spread(1, s_ref[1])
    re = re1 * re0 - im1 * im0
    im = re1 * im0 + im1 * re0
    out_im = lax.broadcasted_iota(jnp.int32, (SIDE, SIDE), 0) // SPAN % 2
    in_im = lax.broadcasted_iota(jnp.int32, (SIDE, SIDE), 1) // SPAN % 2
    o_ref[...] = jnp.where(out_im == in_im, re, jnp.where(out_im == 1, im, -im))


def superop_matrix(layer_super, by_row):
    return pl.pallas_call(
        functools.partial(superop_body, by_row),
        out_shape=jax.ShapeDtypeStruct((SIDE, SIDE), jnp.float32),
        in_specs=[whole()],
        out_specs=whole(),
        compiler_params=params(),
        cost_estimate=cost(10**8, 10**6),
        name="superop",
    )(layer_super)


def turn_body(x_ref, o_ref):
    parts = x_ref.shape[0] // LANES
    cols = x_ref.shape[1]
    for k in range(parts):
        o_ref[pl.ds(k, cols, stride=parts), :] = x_ref[pl.ds(k * LANES, LANES), :].T


def turn_order_body(order_ref, x_ref, o_ref):
    parts = x_ref.shape[0] // LANES
    cols = x_ref.shape[1]
    half = parts // 2
    order = order_ref[...].astype(jnp.bfloat16)
    for part in range(2):
        x = reorder(order, x_ref[pl.ds(part * half * LANES, half * LANES), :])
        for k in range(half):
            o_ref[pl.ds(k * 2 + part, cols, stride=parts), :] = x[k * LANES : (k + 1) * LANES].T


def turn(x, order=None):
    height, full = x.shape
    parts = height // LANES
    cols = 512
    extra = [] if order is None else [order]
    return pl.pallas_call(
        turn_body if order is None else turn_order_body,
        out_shape=jax.ShapeDtypeStruct((full * parts, LANES), x.dtype),
        grid=(full // cols,),
        in_specs=[pl.BlockSpec(o.shape, lambda i: (0, 0)) for o in extra]
        + [pl.BlockSpec((height, cols), lambda i: (0, i))],
        out_specs=pl.BlockSpec((cols * parts, LANES), lambda i: (i, 0)),
        compiler_params=params(),
        cost_estimate=cost(10**8, 2 * x.size * 4),
        name="turn",
    )(*extra, x)


def pick_body(group, share, devices, parts, idx_ref, x_ref, o_ref):
    count = share // GROUPS
    targets = o_ref.shape[0]
    senders = x_ref.shape[0] // (parts * idx_ref.shape[0])
    start = pl.program_id(0) * targets

    @pl.loop(0, targets)
    def _(i):
        d = start + i
        first = d % devices * share + group * count
        skip = d // devices * parts
        copy_rows(idx_ref, first, 1, count, parts, x_ref, o_ref.at[i], 0, senders * parts, skip)


def pick(xt, table, group, devices, parts):
    full = table.shape[0]
    share = full // devices
    targets = devices * (xt.shape[0] // (full * parts))
    steps = 4
    rows = share // GROUPS * parts
    return pl.pallas_call(
        functools.partial(pick_body, group, share, devices, parts),
        out_shape=jax.ShapeDtypeStruct((targets, rows, LANES), xt.dtype),
        grid_spec=pltpu.PrefetchScalarGridSpec(
            num_scalar_prefetch=1,
            grid=(steps,),
            in_specs=[whole()],
            out_specs=pl.BlockSpec((targets // steps, rows, LANES), lambda i, s: (i, 0, 0)),
        ),
        compiler_params=params(),
        cost_estimate=cost(10**8, 3 * xt.size * 4),
        name="pick",
    )(table, xt)


def mix(idx_ref, w_ref, g, xk, tmp):
    high = tmp.shape[0] // 2
    groups = LANES // SPAN

    @pl.loop(0, SPAN)
    def _(low):
        copy_rows(idx_ref, low, SPAN, high, 2, g, tmp, 0)
        for part in range(2):
            turned = tmp[pl.ds(part, high, stride=2), :].T
            at = pl.multiple_of(low * 2 * SPAN + part * SPAN, SPAN)
            xk[:, pl.ds(at, SPAN), :] = turned.reshape(groups, SPAN, high)

    w_big, w_small = two_parts(w_ref[...])

    @pl.loop(0, groups)
    def _(group):
        x_big, x_small = two_parts(xk[group])
        y = jnp.dot(w_big, x_small, preferred_element_type=jnp.float32)
        y += jnp.dot(w_small, x_big, preferred_element_type=jnp.float32)
        y += jnp.dot(w_big, x_big, preferred_element_type=jnp.float32)
        xk[group] = y


def middle_body(chunks, count, blocks, idx_ref, next_ref, w_ref, r_ref, *refs):
    *outs, g, xk, tmp = refs
    sources = r_ref.shape[0]
    parts = r_ref.shape[1] // (LANES * chunks)
    halves = parts // 2
    local = halves * LANES
    high = tmp.shape[0] // 2
    rows = next_ref.shape[0] // (outs[0].shape[0] * blocks)

    @pl.loop(0, chunks)
    def _(c):
        @pl.loop(0, sources)
        def _(s):
            for k in range(parts):
                part, half = k // halves, k % halves
                block = r_ref[s, pl.ds(c * (LANES * parts) + k, LANES, stride=parts), :]
                at = (s * local + half * LANES) * 2 + part
                g[pl.ds(at, LANES, stride=2), :] = block.T

        mix(idx_ref, w_ref, g, xk, tmp)

        @pl.loop(0, SPAN)
        def _(low):
            for part in range(2):
                at = pl.multiple_of(low * 2 * SPAN + part * SPAN, SPAN)
                block = xk[:, pl.ds(at, SPAN), :].reshape(LANES, high)
                g[pl.ds(low * high * 2 + part, high, stride=2), :] = block.T

        @pl.loop(0, outs[0].shape[0])
        def _(d):
            for b in range(blocks):
                out, base = (outs[0], (c * blocks + b) * rows) if count == 1 else (outs[b], c * rows)
                copy_rows(next_ref, (d * blocks + b) * rows, 1, rows, 2, g, out.at[d], base)


def middle(r, table, next_table, w, chunks, devices, blocks, split):
    full = table.shape[0]
    high = full // SPAN
    count = blocks if split else 1
    rows = next_table.shape[0] // (devices * blocks) * chunks * (blocks // count)
    message = jax.ShapeDtypeStruct((devices, 2 * rows, LANES), r.dtype)
    return pl.pallas_call(
        functools.partial(middle_body, chunks, count, blocks),
        out_shape=[message] * count,
        in_specs=[scalars(), scalars(), whole(), whole()],
        out_specs=[whole()] * count,
        scratch_shapes=[
            pltpu.VMEM((full * 2, LANES), r.dtype),
            pltpu.VMEM((LANES // SPAN, SIDE, high), r.dtype),
            pltpu.VMEM((high * 2, LANES), r.dtype),
        ],
        compiler_params=params(),
        cost_estimate=cost(2 * 3 * SIDE * r.size, 2 * r.size * 4),
        name="middle",
    )(table, next_table, w, r)


def last_body(chunks, which, blocks, paired, idx_ref, mine_ref, w_ref, *refs):
    if paired:
        order_ref, *refs = refs
    rs = refs[:GROUPS]
    o_ref, t_ref, g, xk, tmp = refs[-5:]
    full = idx_ref.shape[0]
    high = tmp.shape[0] // 2
    step = pl.program_id(0)
    sources = rs[0].shape[0] // (2 if paired else 1)
    rows = LANES // (2 if paired else 1)
    share = full // sources

    @pl.when(step == 0)
    def _():
        if paired:
            order = order_ref[...].astype(jnp.bfloat16)

        @pl.loop(0, sources)
        def _(s):
            for a, r_ref in enumerate(rs):
                there = blocks if r_ref.shape[1] == 2 * rows * chunks * blocks else 1
                for c in range(chunks):
                    for part in range(2):
                        base = (c * there + (which if there > 1 else 0)) * rows * 2 + part
                        at = pl.ds(base, rows, stride=2)
                        if paired:
                            block = jnp.concatenate([r_ref[s, at, :], r_ref[s + sources, at, :]])
                            block = reorder(order, block)
                        else:
                            block = r_ref[s, at, :]
                        to = (s * share + (a * chunks + c) * LANES) * 2 + part
                        g[pl.ds(to, LANES, stride=2), :] = block.T

        mix(idx_ref, w_ref, g, xk, tmp)

        @pl.loop(0, SPAN)
        def _(low):
            for part in range(2):
                at = pl.multiple_of(low * 2 * SPAN + part * SPAN, SPAN)
                block = xk[:, pl.ds(at, SPAN), :].reshape(LANES, high)
                g[pl.ds(part * full + low, high, stride=SPAN), :] = block.T

    cols = o_ref.shape[2]
    for part in range(2):
        at = pl.multiple_of(part * full + step * cols, LANES)
        o_ref[part] = g[pl.ds(at, cols), :].T

    diagonal = mine_ref[0] + which * LANES

    @pl.when(step == diagonal // cols)
    def _():
        square = o_ref[0, :, pl.ds(pl.multiple_of(diagonal % cols, LANES), LANES)]
        row = lax.broadcasted_iota(jnp.int32, square.shape, 0)
        col = lax.broadcasted_iota(jnp.int32, square.shape, 1)
        mine = jnp.sum(jnp.where(row == col, square, 0.0), axis=0, keepdims=True)
        t_ref[...] = mine + refs[GROUPS][...] if which else mine


def last(rs, table, mine, w, order, chunks, which, blocks, before):
    full = table.shape[0]
    high = full // SPAN
    cols = 1024
    orders = [] if order is None else [order]
    ins = [table, mine, w, *orders, *rs]
    return pl.pallas_call(
        functools.partial(last_body, chunks, which, blocks, order is not None),
        out_shape=(
            jax.ShapeDtypeStruct((2, blocks * LANES, full), rs[0].dtype),
            jax.ShapeDtypeStruct((1, LANES), rs[0].dtype),
        ),
        grid=(full // cols,),
        in_specs=[scalars()] * 2
        + [whole()] * (len(ins) - 2)
        + [whole(), pl.BlockSpec(memory_space=pl.ANY)][: len(before)],
        out_specs=(
            pl.BlockSpec((2, LANES, cols), lambda i: (0, which, i)),
            pl.BlockSpec((1, LANES), lambda i: (0, 0)),
        ),
        scratch_shapes=[
            pltpu.VMEM((full * 2, LANES), rs[0].dtype),
            pltpu.VMEM((LANES // SPAN, SIDE, high), rs[0].dtype),
            pltpu.VMEM((high * 2, LANES), rs[0].dtype),
        ],
        input_output_aliases={len(ins) + 1: 0} if before else {},
        compiler_params=params(),
        cost_estimate=cost(2 * 3 * SIDE * full * 2 * LANES, 4 * full * 2 * LANES * 4),
        name="last",
    )(*ins, *before[::-1])


def sum_over_devices(value, devices):
    return jnp.sum(exchange(jnp.broadcast_to(value, (devices, value.shape[1]))))


def after(x, *done):
    return lax.optimization_barrier((x, *done))[0]


def bit_in(x, at):
    low = jnp.left_shift(1, at) - 1
    return jnp.left_shift(x - (x & low), 1) + (x & low)


def bit_out(x, at):
    low = jnp.left_shift(1, at) - 1
    return jnp.left_shift(jnp.right_shift(x, at + 1), at) + (x & low)


def spread(q, count):
    return q % SPAN * (count // SPAN) + q // SPAN


def run_plan(plan, rho, perm, superop, marks, devices):
    full = rho.shape[2]
    local = full // devices
    blocks = local // LANES
    top = full // 2
    half = devices // 2
    halves = [list(range(half)), list(range(half, devices))]
    table0 = relabel_table(perm[0], full)
    kept, place, final, source = (marks[k] for k in range(4))
    x = rho.reshape(2 * local, full)
    q = jnp.arange(top, dtype=jnp.int32)
    first_groups = second_groups = order = None

    if plan == "full":
        share, parts, chunks = devices, 2 * blocks, 1
        xt = turn(x)
        rows0 = table0
        rows1 = spread(relabel_table(perm[1], full), full)
        targets = devices
    else:
        share, chunks = half, 2
        if plan == "send_keep":
            parts = 2
            at = jnp.arange(local, dtype=jnp.int32)
            new = bit_out(at, source) + (jnp.right_shift(at, source) & 1) * (local // 2)
            xt = turn(x, jnp.where(at[:, None] == new[None, :], 1.0, 0.0))
            old = relabel(bit_in(q, final), perm[0])
            rows0 = old // local * (local // 2) + bit_out(old % local, source)
            stays = final
        else:
            parts = 2 * blocks
            first_groups = halves
            xt = turn(x)
            rows0 = relabel(bit_in(q, kept), perm[0])
            stays = kept
        if plan == "keep_send":
            targets = devices
            few = LANES // 2
            row = q // few * LANES + bit_in(q % few, place)
            at = jnp.arange(LANES, dtype=jnp.int32)
            sent = bit_in(at % few, place) + jnp.left_shift(at // few, place)
            order = jnp.where(at[:, None] == sent[None, :], 1.0, 0.0)
        else:
            targets = half
            second_groups = halves
            row = q
        rows1 = spread(bit_out(relabel(row, perm[1]), stays), top)

    table1 = relabel_table(perm[1], full)
    got = []
    for a in range(GROUPS):
        message = pick(xt, table0, a, share, parts)
        got.append(exchange(after(message, *got[-1:]), first_groups))
    kernel0 = superop_matrix(superop[0], True)
    kernel1 = superop_matrix(superop[1], False)
    done = got[-1]
    parts_of = [[] for _ in range(blocks)]
    for a in range(GROUPS):
        split = a == GROUPS - 1
        messages = middle(got[a], rows0, rows1, kernel0, chunks, targets, blocks, split)
        arrived = []
        for message in messages:
            done = exchange(after(message, done), second_groups)
            arrived.append(done)
        for b in range(blocks):
            parts_of[b].append(arrived[b] if split else arrived[0])
    done = ()
    mine = jnp.reshape(lax.axis_index(AXES).astype(jnp.int32) * local, (1,))
    for b in range(blocks):
        done = last(parts_of[b], table1, mine, kernel1, order, chunks, b, blocks, done)
    return done


def mark_bits(perm):
    qubits = jnp.arange(perm.shape[1], dtype=jnp.int32)
    kept = jnp.sum(jnp.where(perm[0] == qubits[-1], qubits, 0))
    place = jnp.sum(jnp.where(perm[1] == kept, qubits, 0))
    final = perm[1][-1]
    source = jnp.sum(jnp.where(qubits == final, perm[0], 0))
    return jnp.stack([kept, place, final, source])


def choose_plan(marks, local, top_bit):
    low_bits = (SPAN - 1).bit_length()
    kept, place, final, source = (marks[k] for k in range(4))
    plain = kept >= low_bits
    keep_send = plain & (place < LANES.bit_length() - 1)
    keep_keep = plain & (place == top_bit)
    send_keep = (final >= low_bits) & (source < local.bit_length() - 1)
    return jnp.where(keep_send, 1, jnp.where(keep_keep, 2, jnp.where(send_keep, 3, 0)))


def chunked_per_device(rho, perm, superop):
    full = rho.shape[2]
    local = rho.shape[1]
    devices = full // local
    plans = ("full", "keep_send", "keep_keep", "send_keep")
    runs = [functools.partial(run_plan, plan, devices=devices) for plan in plans]
    marks = mark_bits(perm)
    plan = choose_plan(marks, local, perm.shape[1] - 1)
    return lax.switch(plan, runs, rho, perm, superop, marks)


def per_device(rho, perm, superop):
    full = rho.shape[2]
    local = rho.shape[1]
    if local == GROUPS * LANES:
        matrix, diagonal = chunked_per_device(rho, perm, superop)
    else:
        matrix = simple_per_device(rho, perm, superop)
        position = lax.axis_index(AXES)
        block = lax.dynamic_slice_in_dim(matrix[0], position * local, local, 1)
        diagonal = jnp.broadcast_to(jnp.trace(block) / LANES, (1, LANES))
    return (matrix, sum_over_devices(diagonal, full // local) / full)


def solution(mesh):
    assert PAIRS == 2
    placed = (P(None, AXES, None), P(), P())
    return jax.shard_map(
        per_device,
        mesh=mesh,
        in_specs=placed,
        out_specs=(P(None, AXES, None), P()),
        check_vma=False,
    )
```

```python
import functools

import jax
import jax.numpy as jnp
from jax import lax
from jax.experimental import pallas as pl
from jax.experimental.pallas import tpu as pltpu
from jax.sharding import PartitionSpec as P

PAIRS = 2
SPAN = 4**PAIRS
AXES = ("hi", "grp")
VMEM_LIMIT = 60 * 1024 * 1024
LANES = 128
SIDE = 2 * SPAN * SPAN
GROUPS = 2


def relabel_table(order, count):
    return relabel(jnp.arange(count, dtype=jnp.int32), order)


def relabel(positions, order):
    qubits = jnp.arange(order.shape[0], dtype=jnp.int32)[:, None]
    bits = jnp.right_shift(positions[None, :], qubits) & 1
    return jnp.sum(jnp.left_shift(bits, order[:, None]), axis=0)


def gather_body(idx_ref, x_ref, o_ref):
    rows = o_ref.shape[0]
    base = pl.program_id(0) * rows

    @pl.loop(0, rows // 8)
    def _(block):
        start = pl.multiple_of(block * 8, 8)
        for k in range(8):
            src = idx_ref[base + start + k]
            o_ref[pl.ds(start + k, 1), :] = x_ref[pl.ds(src, 1), :]


def gather_rows(x, idx):
    count, width = x.shape
    rows = 512
    return pl.pallas_call(
        gather_body,
        out_shape=jax.ShapeDtypeStruct(x.shape, x.dtype),
        grid_spec=pltpu.PrefetchScalarGridSpec(
            num_scalar_prefetch=1,
            grid=(count // rows,),
            in_specs=[
                pl.BlockSpec((count, width), lambda i, s: (0, 0), pipeline_mode=pl.Buffered(1))
            ],
            out_specs=pl.BlockSpec((rows, width), lambda i, s: (i, 0)),
        ),
        compiler_params=pltpu.CompilerParams(vmem_limit_bytes=VMEM_LIMIT),
        name="gather_rows",
    )(idx, x)


def gather_turn_body(idx_ref, x_ref, o_ref, tmp):
    rows = tmp.shape[0]
    low = pl.program_id(0)

    @pl.loop(0, rows // 8)
    def _(block):
        start = pl.multiple_of(block * 8, 8)
        for k in range(8):
            src = idx_ref[(start + k) * SPAN + low]
            tmp[pl.ds(start + k, 1), :] = x_ref[pl.ds(src, 1), :]

    o_ref[0] = tmp[...].T


def gather_turn(x, idx):
    count, width = x.shape
    rows = count // SPAN
    return pl.pallas_call(
        gather_turn_body,
        out_shape=jax.ShapeDtypeStruct((SPAN, width, rows), x.dtype),
        grid_spec=pltpu.PrefetchScalarGridSpec(
            num_scalar_prefetch=1,
            grid=(SPAN,),
            in_specs=[
                pl.BlockSpec((count, width), lambda i, s: (0, 0), pipeline_mode=pl.Buffered(1))
            ],
            out_specs=pl.BlockSpec((1, width, rows), lambda i, s: (i, 0, 0)),
            scratch_shapes=[pltpu.VMEM((rows, width), x.dtype)],
        ),
        compiler_params=pltpu.CompilerParams(vmem_limit_bytes=VMEM_LIMIT),
        name="gather_turn",
    )(idx, x)


def channel_body(kernel_ref, x_ref, o_ref):
    block = x_ref[...].reshape(2 * SPAN * SPAN, x_ref.shape[-1])
    mixed = jnp.dot(
        kernel_ref[...],
        block,
        precision=lax.Precision.HIGHEST,
        preferred_element_type=jnp.float32,
    )
    o_ref[...] = mixed.reshape(o_ref.shape)


def apply_channel(x, kernel):
    span, width, lanes = x.shape
    blocks = width // (2 * SPAN)
    shaped = x.reshape(span, 2, blocks, SPAN, lanes)
    side = 2 * SPAN * SPAN
    spec = pl.BlockSpec((span, 2, 1, SPAN, lanes), lambda i: (0, 0, i, 0, 0))
    whole = pl.BlockSpec((side, side), lambda i: (0, 0))
    out = pl.pallas_call(
        channel_body,
        out_shape=jax.ShapeDtypeStruct(shaped.shape, x.dtype),
        grid=(blocks,),
        in_specs=[whole, spec],
        out_specs=spec,
        compiler_params=pltpu.CompilerParams(vmem_limit_bytes=VMEM_LIMIT),
        name="channel",
    )(kernel, shaped)
    return out.reshape(x.shape)


def pair_kernel(layer_super):
    real = layer_super[0].reshape(4, 4, 4, 4)
    imag = layer_super[1].reshape(4, 4, 4, 4)

    def outer(a, b):
        both = a[:, None, :, None, :, None, :, None] * b[None, :, None, :, None, :, None, :]
        return both.reshape(SPAN, SPAN, SPAN, SPAN)

    re = outer(real, real) - outer(imag, imag)
    im = outer(real, imag) + outer(imag, real)
    top = jnp.stack([re, -im], axis=2)
    bottom = jnp.stack([im, re], axis=2)
    return jnp.stack([top, bottom], axis=0)


def exchange(x, groups=None):
    return lax.all_to_all(
        x, AXES, split_axis=0, concat_axis=0, tiled=True, axis_index_groups=groups
    )


def swap_local(x, local):
    shaped = x.reshape(x.shape[0] // local, local, 2, local)
    return jnp.transpose(shaped, (0, 3, 2, 1)).reshape(x.shape)


def simple_per_device(rho, perm, superop):
    full = rho.shape[2]
    local = rho.shape[1]
    side = 2 * SPAN * SPAN
    table0 = relabel_table(perm[0], full)
    table1 = relabel_table(perm[1], full)
    kernel0 = jnp.transpose(pair_kernel(superop[0]), (1, 0, 2, 4, 3, 5)).reshape(side, side)
    kernel1 = jnp.transpose(pair_kernel(superop[1]), (2, 0, 1, 5, 3, 4)).reshape(side, side)

    x = rho.reshape(2 * local, full).T
    x = gather_rows(x, table0)
    x = exchange(x)
    x = swap_local(x, local)
    x = gather_turn(x, table0)
    x = apply_channel(x, kernel0)
    x = jnp.transpose(x, (2, 0, 1)).reshape(full, 2 * local)
    x = gather_rows(x, table1)
    x = exchange(x)
    x = swap_local(x, local)
    x = gather_turn(x, table1)
    x = apply_channel(x, kernel1)
    x = jnp.transpose(x, (2, 0, 1)).reshape(full, 2 * local)
    matrix = x.T.reshape(2, local, full)

    return matrix


def params():
    return pltpu.CompilerParams(vmem_limit_bytes=VMEM_LIMIT)


def cost(flops, nbytes):
    return pl.CostEstimate(flops=flops, bytes_accessed=nbytes, transcendentals=0)


def whole():
    return pl.BlockSpec(memory_space=pltpu.VMEM)


def scalars():
    return pl.BlockSpec(memory_space=pltpu.SMEM)


def two_parts(x):
    big = x.astype(jnp.bfloat16)
    return big, (x - big.astype(jnp.float32)).astype(jnp.bfloat16)


def reorder(order, x):
    big, small = two_parts(x)
    y = jnp.dot(order, small, preferred_element_type=jnp.float32)
    return y + jnp.dot(order, big, preferred_element_type=jnp.float32)


def copy_rows(idx_ref, first, step, count, parts, src_ref, dst_ref, base, whole_row=None, skip=0):
    pitch = parts if whole_row is None else whole_row
    near = [idx_ref[step * k] * pitch for k in range(8)]

    @pl.loop(0, count // 16)
    def _(block):
        start = block * 16
        for far in range(0, 16, 8):
            origin = idx_ref[first + step * (start + far)] * pitch + skip
            for k in range(8):
                src = pl.multiple_of(origin + near[k], parts)
                dst = pl.multiple_of((base + start + far + k) * parts, parts)
                dst_ref[pl.ds(dst, parts), :] = src_ref[pl.ds(src, parts), :]


def superop_body(by_row, s_ref, o_ref):
    at = lax.broadcasted_iota(jnp.int32, (SIDE, SPAN), 0)
    entry = lax.broadcasted_iota(jnp.int32, (SIDE, SPAN), 1)
    first, last_ = at // (2 * SPAN), at % SPAN
    row, col = (first, last_) if by_row else (last_, first)

    def spread(pair, values):
        mine = jnp.right_shift(row, 2 * pair) % 4 * 4 + jnp.right_shift(col, 2 * pair) % 4
        pick_ = jnp.where(mine == entry, 1.0, 0.0)
        rows = jnp.dot(
            pick_, values, precision=lax.Precision.HIGHEST, preferred_element_type=jnp.float32
        )
        return lax.dot_general(
            rows,
            pick_,
            (((1,), (1,)), ((), ())),
            precision=lax.Precision.HIGHEST,
            preferred_element_type=jnp.float32,
        )

    re0, im0 = spread(0, s_ref[0]), spread(0, s_ref[1])
    re1, im1 = spread(1, s_ref[0]), spread(1, s_ref[1])
    re = re1 * re0 - im1 * im0
    im = re1 * im0 + im1 * re0
    out_im = lax.broadcasted_iota(jnp.int32, (SIDE, SIDE), 0) // SPAN % 2
    in_im = lax.broadcasted_iota(jnp.int32, (SIDE, SIDE), 1) // SPAN % 2
    o_ref[...] = jnp.where(out_im == in_im, re, jnp.where(out_im == 1, im, -im))


def superop_matrix(layer_super, by_row):
    return pl.pallas_call(
        functools.partial(superop_body, by_row),
        out_shape=jax.ShapeDtypeStruct((SIDE, SIDE), jnp.float32),
        in_specs=[whole()],
        out_specs=whole(),
        compiler_params=params(),
        cost_estimate=cost(10**8, 10**6),
        name="superop",
    )(layer_super)


def turn_body(x_ref, o_ref):
    parts = x_ref.shape[0] // LANES
    cols = x_ref.shape[1]
    for k in range(parts):
        o_ref[pl.ds(k, cols, stride=parts), :] = x_ref[pl.ds(k * LANES, LANES), :].T


def turn_order_body(order_ref, x_ref, o_ref):
    parts = x_ref.shape[0] // LANES
    cols = x_ref.shape[1]
    half = parts // 2
    order = order_ref[...].astype(jnp.bfloat16)
    for part in range(2):
        x = reorder(order, x_ref[pl.ds(part * half * LANES, half * LANES), :])
        for k in range(half):
            o_ref[pl.ds(k * 2 + part, cols, stride=parts), :] = x[k * LANES : (k + 1) * LANES].T


def turn(x, order=None):
    height, full = x.shape
    parts = height // LANES
    cols = 512
    extra = [] if order is None else [order]
    return pl.pallas_call(
        turn_body if order is None else turn_order_body,
        out_shape=jax.ShapeDtypeStruct((full * parts, LANES), x.dtype),
        grid=(full // cols,),
        in_specs=[pl.BlockSpec(o.shape, lambda i: (0, 0)) for o in extra]
        + [pl.BlockSpec((height, cols), lambda i: (0, i))],
        out_specs=pl.BlockSpec((cols * parts, LANES), lambda i: (i, 0)),
        compiler_params=params(),
        cost_estimate=cost(10**8, 2 * x.size * 4),
        name="turn",
    )(*extra, x)


def pick_body(groups, share, devices, parts, idx_ref, x_ref, *outs):
    count = share // GROUPS
    targets = outs[0].shape[0]
    senders = x_ref.shape[0] // (parts * idx_ref.shape[0])
    start = pl.program_id(0) * targets

    @pl.loop(0, targets)
    def _(i):
        d = start + i
        skip = d // devices * parts
        for group, out in zip(groups, outs):
            first = d % devices * share + group * count
            copy_rows(idx_ref, first, 1, count, parts, x_ref, out.at[i], 0, senders * parts, skip)


def pick(xt, table, groups, devices, parts):
    full = table.shape[0]
    share = full // devices
    targets = devices * (xt.shape[0] // (full * parts))
    steps = 4
    rows = share // GROUPS * parts
    spec = pl.BlockSpec((targets // steps, rows, LANES), lambda i, s: (i, 0, 0))
    return pl.pallas_call(
        functools.partial(pick_body, groups, share, devices, parts),
        out_shape=[jax.ShapeDtypeStruct((targets, rows, LANES), xt.dtype)] * len(groups),
        grid_spec=pltpu.PrefetchScalarGridSpec(
            num_scalar_prefetch=1, grid=(steps,), in_specs=[whole()], out_specs=[spec] * len(groups)
        ),
        compiler_params=params(),
        cost_estimate=cost(10**8, 3 * xt.size * 4),
        name="pick",
    )(table, xt)


def mix(idx_ref, w_ref, g, xk, tmp):
    high = tmp.shape[0] // 2
    groups = LANES // SPAN

    @pl.loop(0, SPAN)
    def _(low):
        copy_rows(idx_ref, low, SPAN, high, 2, g, tmp, 0)
        for part in range(2):
            turned = tmp[pl.ds(part, high, stride=2), :].T
            at = pl.multiple_of(low * 2 * SPAN + part * SPAN, SPAN)
            xk[:, pl.ds(at, SPAN), :] = turned.reshape(groups, SPAN, high)

    w_big, w_small = two_parts(w_ref[...])

    @pl.loop(0, groups)
    def _(group):
        x_big, x_small = two_parts(xk[group])
        y = jnp.dot(w_big, x_small, preferred_element_type=jnp.float32)
        y += jnp.dot(w_small, x_big, preferred_element_type=jnp.float32)
        y += jnp.dot(w_big, x_big, preferred_element_type=jnp.float32)
        xk[group] = y


def middle_body(chunks, count, blocks, idx_ref, next_ref, w_ref, r_ref, *refs):
    *outs, g, xk, tmp = refs
    sources = r_ref.shape[0]
    parts = r_ref.shape[1] // (LANES * chunks)
    halves = parts // 2
    local = halves * LANES
    high = tmp.shape[0] // 2
    rows = next_ref.shape[0] // (outs[0].shape[0] * blocks)

    @pl.loop(0, chunks)
    def _(c):
        @pl.loop(0, sources)
        def _(s):
            for k in range(parts):
                part, half = k // halves, k % halves
                block = r_ref[s, pl.ds(c * (LANES * parts) + k, LANES, stride=parts), :]
                at = (s * local + half * LANES) * 2 + part
                g[pl.ds(at, LANES, stride=2), :] = block.T

        mix(idx_ref, w_ref, g, xk, tmp)

        @pl.loop(0, SPAN)
        def _(low):
            for part in range(2):
                at = pl.multiple_of(low * 2 * SPAN + part * SPAN, SPAN)
                block = xk[:, pl.ds(at, SPAN), :].reshape(LANES, high)
                g[pl.ds(low * high * 2 + part, high, stride=2), :] = block.T

        @pl.loop(0, outs[0].shape[0])
        def _(d):
            for b in range(blocks):
                out, base = (outs[0], (c * blocks + b) * rows) if count == 1 else (outs[b], c * rows)
                copy_rows(next_ref, (d * blocks + b) * rows, 1, rows, 2, g, out.at[d], base)


def middle(r, table, next_table, w, chunks, devices, blocks, split):
    full = table.shape[0]
    high = full // SPAN
    count = blocks if split else 1
    rows = next_table.shape[0] // (devices * blocks) * chunks * (blocks // count)
    message = jax.ShapeDtypeStruct((devices, 2 * rows, LANES), r.dtype)
    return pl.pallas_call(
        functools.partial(middle_body, chunks, count, blocks),
        out_shape=[message] * count,
        in_specs=[scalars(), scalars(), whole(), whole()],
        out_specs=[whole()] * count,
        scratch_shapes=[
            pltpu.VMEM((full * 2, LANES), r.dtype),
            pltpu.VMEM((LANES // SPAN, SIDE, high), r.dtype),
            pltpu.VMEM((high * 2, LANES), r.dtype),
        ],
        compiler_params=params(),
        cost_estimate=cost(2 * 3 * SIDE * r.size, 2 * r.size * 4),
        name="middle",
    )(table, next_table, w, r)


def last_body(chunks, which, blocks, paired, idx_ref, mine_ref, w_ref, *refs):
    if paired:
        order_ref, *refs = refs
    rs = refs[:GROUPS]
    o_ref, t_ref, g, xk, tmp = refs[-5:]
    full = idx_ref.shape[0]
    high = tmp.shape[0] // 2
    step = pl.program_id(0)
    sources = rs[0].shape[0] // (2 if paired else 1)
    rows = LANES // (2 if paired else 1)
    share = full // sources

    @pl.when(step == 0)
    def _():
        if paired:
            order = order_ref[...].astype(jnp.bfloat16)

        @pl.loop(0, sources)
        def _(s):
            for a, r_ref in enumerate(rs):
                there = blocks if r_ref.shape[1] == 2 * rows * chunks * blocks else 1
                for c in range(chunks):
                    for part in range(2):
                        base = (c * there + (which if there > 1 else 0)) * rows * 2 + part
                        at = pl.ds(base, rows, stride=2)
                        if paired:
                            block = jnp.concatenate([r_ref[s, at, :], r_ref[s + sources, at, :]])
                            block = reorder(order, block)
                        else:
                            block = r_ref[s, at, :]
                        to = (s * share + (a * chunks + c) * LANES) * 2 + part
                        g[pl.ds(to, LANES, stride=2), :] = block.T

        mix(idx_ref, w_ref, g, xk, tmp)

        @pl.loop(0, SPAN)
        def _(low):
            for part in range(2):
                at = pl.multiple_of(low * 2 * SPAN + part * SPAN, SPAN)
                block = xk[:, pl.ds(at, SPAN), :].reshape(LANES, high)
                g[pl.ds(part * full + low, high, stride=SPAN), :] = block.T

    cols = o_ref.shape[2]
    for part in range(2):
        at = pl.multiple_of(part * full + step * cols, LANES)
        o_ref[part] = g[pl.ds(at, cols), :].T

    diagonal = mine_ref[0] + which * LANES

    @pl.when(step == diagonal // cols)
    def _():
        square = o_ref[0, :, pl.ds(pl.multiple_of(diagonal % cols, LANES), LANES)]
        row = lax.broadcasted_iota(jnp.int32, square.shape, 0)
        col = lax.broadcasted_iota(jnp.int32, square.shape, 1)
        mine = jnp.sum(jnp.where(row == col, square, 0.0), axis=0, keepdims=True)
        t_ref[...] = mine + refs[GROUPS][...] if which else mine


def last(rs, table, mine, w, order, chunks, which, blocks, before):
    full = table.shape[0]
    high = full // SPAN
    cols = 1024
    orders = [] if order is None else [order]
    ins = [table, mine, w, *orders, *rs]
    return pl.pallas_call(
        functools.partial(last_body, chunks, which, blocks, order is not None),
        out_shape=(
            jax.ShapeDtypeStruct((2, blocks * LANES, full), rs[0].dtype),
            jax.ShapeDtypeStruct((1, LANES), rs[0].dtype),
        ),
        grid=(full // cols,),
        in_specs=[scalars()] * 2
        + [whole()] * (len(ins) - 2)
        + [whole(), pl.BlockSpec(memory_space=pl.ANY)][: len(before)],
        out_specs=(
            pl.BlockSpec((2, LANES, cols), lambda i: (0, which, i)),
            pl.BlockSpec((1, LANES), lambda i: (0, 0)),
        ),
        scratch_shapes=[
            pltpu.VMEM((full * 2, LANES), rs[0].dtype),
            pltpu.VMEM((LANES // SPAN, SIDE, high), rs[0].dtype),
            pltpu.VMEM((high * 2, LANES), rs[0].dtype),
        ],
        input_output_aliases={len(ins) + 1: 0} if before else {},
        compiler_params=params(),
        cost_estimate=cost(2 * 3 * SIDE * full * 2 * LANES, 4 * full * 2 * LANES * 4),
        name="last",
    )(*ins, *before[::-1])


def sum_over_devices(value, devices):
    return jnp.sum(exchange(jnp.broadcast_to(value, (devices, value.shape[1]))))


def after(x, *done):
    return lax.optimization_barrier((x, *done))[0]


def bit_in(x, at):
    low = jnp.left_shift(1, at) - 1
    return jnp.left_shift(x - (x & low), 1) + (x & low)


def bit_out(x, at):
    low = jnp.left_shift(1, at) - 1
    return jnp.left_shift(jnp.right_shift(x, at + 1), at) + (x & low)


def spread(q, count):
    return q % SPAN * (count // SPAN) + q // SPAN


def run_plan(plan, rho, perm, superop, marks, devices):
    full = rho.shape[2]
    local = full // devices
    blocks = local // LANES
    top = full // 2
    half = devices // 2
    halves = [list(range(half)), list(range(half, devices))]
    table0 = relabel_table(perm[0], full)
    kept, place, final, source = (marks[k] for k in range(4))
    x = rho.reshape(2 * local, full)
    q = jnp.arange(top, dtype=jnp.int32)
    first_groups = second_groups = order = None

    if plan == "full":
        share, parts, chunks = devices, 2 * blocks, 1
        xt = turn(x)
        rows0 = table0
        rows1 = spread(relabel_table(perm[1], full), full)
        targets = devices
    else:
        share, chunks = half, 2
        if plan == "send_keep":
            parts = 2
            at = jnp.arange(local, dtype=jnp.int32)
            new = bit_out(at, source) + (jnp.right_shift(at, source) & 1) * (local // 2)
            xt = turn(x, jnp.where(at[:, None] == new[None, :], 1.0, 0.0))
            old = relabel(bit_in(q, final), perm[0])
            rows0 = old // local * (local // 2) + bit_out(old % local, source)
            stays = final
        else:
            parts = 2 * blocks
            first_groups = halves
            xt = turn(x)
            rows0 = relabel(bit_in(q, kept), perm[0])
            stays = kept
        if plan == "keep_send":
            targets = devices
            few = LANES // 2
            row = q // few * LANES + bit_in(q % few, place)
            at = jnp.arange(LANES, dtype=jnp.int32)
            from_two = bit_in(at % few, place) + jnp.left_shift(at // few, place)
            order = jnp.where(at[:, None] == from_two[None, :], 1.0, 0.0)
        else:
            targets = half
            second_groups = halves
            row = q
        rows1 = spread(bit_out(relabel(row, perm[1]), stays), top)

    table1 = relabel_table(perm[1], full)
    got = []
    if first_groups is None:
        sent = [pick(xt, table0, (a,), share, parts)[0] for a in range(GROUPS)]
        got.append(exchange(sent[0]))
    else:
        sent = pick(xt, table0, tuple(range(GROUPS)), share, parts)
        got.append(exchange(after(*sent), first_groups))
    for message in sent[1:]:
        got.append(exchange(after(message, got[-1]), first_groups))
    kernel0 = superop_matrix(superop[0], True)
    kernel1 = superop_matrix(superop[1], False)
    done = got[-1]
    parts_of = [[] for _ in range(blocks)]
    for a in range(GROUPS):
        split = a == GROUPS - 1
        messages = middle(got[a], rows0, rows1, kernel0, chunks, targets, blocks, split)
        arrived = []
        for message in messages:
            done = exchange(after(message, done), second_groups)
            arrived.append(done)
        for b in range(blocks):
            parts_of[b].append(arrived[b] if split else arrived[0])
    done = ()
    mine = jnp.reshape(lax.axis_index(AXES).astype(jnp.int32) * local, (1,))
    for b in range(blocks):
        done = last(parts_of[b], table1, mine, kernel1, order, chunks, b, blocks, done)
    return done


def mark_bits(perm):
    qubits = jnp.arange(perm.shape[1], dtype=jnp.int32)
    kept = jnp.sum(jnp.where(perm[0] == qubits[-1], qubits, 0))
    place = jnp.sum(jnp.where(perm[1] == kept, qubits, 0))
    final = perm[1][-1]
    source = jnp.sum(jnp.where(qubits == final, perm[0], 0))
    return jnp.stack([kept, place, final, source])


def choose_plan(marks, local, top_bit):
    low_bits = (SPAN - 1).bit_length()
    kept, place, final, source = (marks[k] for k in range(4))
    plain = kept >= low_bits
    keep_send = plain & (place < LANES.bit_length() - 1)
    keep_keep = plain & (place == top_bit)
    send_keep = (final >= low_bits) & (source < local.bit_length() - 1)
    return jnp.where(keep_send, 3, jnp.where(keep_keep, 0, jnp.where(send_keep, 1, 2)))


def chunked_per_device(rho, perm, superop):
    full = rho.shape[2]
    local = rho.shape[1]
    devices = full // local
    plans = ("keep_keep", "send_keep", "full", "keep_send")
    runs = [functools.partial(run_plan, plan, devices=devices) for plan in plans]
    marks = mark_bits(perm)
    plan = choose_plan(marks, local, perm.shape[1] - 1)
    return lax.switch(plan, runs, rho, perm, superop, marks)


def per_device(rho, perm, superop):
    full = rho.shape[2]
    local = rho.shape[1]
    if local == GROUPS * LANES:
        matrix, diagonal = chunked_per_device(rho, perm, superop)
    else:
        matrix = simple_per_device(rho, perm, superop)
        position = lax.axis_index(AXES)
        block = lax.dynamic_slice_in_dim(matrix[0], position * local, local, 1)
        diagonal = jnp.broadcast_to(jnp.trace(block) / LANES, (1, LANES))
    return (matrix, sum_over_devices(diagonal, full // local) / full)


def solution(mesh):
    assert PAIRS == 2
    placed = (P(None, AXES, None), P(), P())
    return jax.shard_map(
        per_device,
        mesh=mesh,
        in_specs=placed,
        out_specs=(P(None, AXES, None), P()),
        check_vma=False,
    )
```

```python
import functools

import jax
import jax.numpy as jnp
from jax import lax
from jax.experimental import pallas as pl
from jax.experimental.pallas import tpu as pltpu
from jax.sharding import PartitionSpec as P

PAIRS = 2
SPAN = 4**PAIRS
AXES = ("hi", "grp")
VMEM_LIMIT = 60 * 1024 * 1024
LANES = 128
SIDE = 2 * SPAN * SPAN
GROUPS = 2


def relabel_table(order, count):
    return relabel(jnp.arange(count, dtype=jnp.int32), order)


def relabel(positions, order):
    qubits = jnp.arange(order.shape[0], dtype=jnp.int32)[:, None]
    bits = jnp.right_shift(positions[None, :], qubits) & 1
    return jnp.sum(jnp.left_shift(bits, order[:, None]), axis=0)


def gather_body(idx_ref, x_ref, o_ref):
    rows = o_ref.shape[0]
    base = pl.program_id(0) * rows

    @pl.loop(0, rows // 8)
    def _(block):
        start = pl.multiple_of(block * 8, 8)
        for k in range(8):
            src = idx_ref[base + start + k]
            o_ref[pl.ds(start + k, 1), :] = x_ref[pl.ds(src, 1), :]


def gather_rows(x, idx):
    count, width = x.shape
    rows = 512
    return pl.pallas_call(
        gather_body,
        out_shape=jax.ShapeDtypeStruct(x.shape, x.dtype),
        grid_spec=pltpu.PrefetchScalarGridSpec(
            num_scalar_prefetch=1,
            grid=(count // rows,),
            in_specs=[
                pl.BlockSpec((count, width), lambda i, s: (0, 0), pipeline_mode=pl.Buffered(1))
            ],
            out_specs=pl.BlockSpec((rows, width), lambda i, s: (i, 0)),
        ),
        compiler_params=pltpu.CompilerParams(vmem_limit_bytes=VMEM_LIMIT),
        name="gather_rows",
    )(idx, x)


def gather_turn_body(idx_ref, x_ref, o_ref, tmp):
    rows = tmp.shape[0]
    low = pl.program_id(0)

    @pl.loop(0, rows // 8)
    def _(block):
        start = pl.multiple_of(block * 8, 8)
        for k in range(8):
            src = idx_ref[(start + k) * SPAN + low]
            tmp[pl.ds(start + k, 1), :] = x_ref[pl.ds(src, 1), :]

    o_ref[0] = tmp[...].T


def gather_turn(x, idx):
    count, width = x.shape
    rows = count // SPAN
    return pl.pallas_call(
        gather_turn_body,
        out_shape=jax.ShapeDtypeStruct((SPAN, width, rows), x.dtype),
        grid_spec=pltpu.PrefetchScalarGridSpec(
            num_scalar_prefetch=1,
            grid=(SPAN,),
            in_specs=[
                pl.BlockSpec((count, width), lambda i, s: (0, 0), pipeline_mode=pl.Buffered(1))
            ],
            out_specs=pl.BlockSpec((1, width, rows), lambda i, s: (i, 0, 0)),
            scratch_shapes=[pltpu.VMEM((rows, width), x.dtype)],
        ),
        compiler_params=pltpu.CompilerParams(vmem_limit_bytes=VMEM_LIMIT),
        name="gather_turn",
    )(idx, x)


def channel_body(kernel_ref, x_ref, o_ref):
    block = x_ref[...].reshape(2 * SPAN * SPAN, x_ref.shape[-1])
    mixed = jnp.dot(
        kernel_ref[...],
        block,
        precision=lax.Precision.HIGHEST,
        preferred_element_type=jnp.float32,
    )
    o_ref[...] = mixed.reshape(o_ref.shape)


def apply_channel(x, kernel):
    span, width, lanes = x.shape
    blocks = width // (2 * SPAN)
    shaped = x.reshape(span, 2, blocks, SPAN, lanes)
    side = 2 * SPAN * SPAN
    spec = pl.BlockSpec((span, 2, 1, SPAN, lanes), lambda i: (0, 0, i, 0, 0))
    whole = pl.BlockSpec((side, side), lambda i: (0, 0))
    out = pl.pallas_call(
        channel_body,
        out_shape=jax.ShapeDtypeStruct(shaped.shape, x.dtype),
        grid=(blocks,),
        in_specs=[whole, spec],
        out_specs=spec,
        compiler_params=pltpu.CompilerParams(vmem_limit_bytes=VMEM_LIMIT),
        name="channel",
    )(kernel, shaped)
    return out.reshape(x.shape)


def pair_kernel(layer_super):
    real = layer_super[0].reshape(4, 4, 4, 4)
    imag = layer_super[1].reshape(4, 4, 4, 4)

    def outer(a, b):
        both = a[:, None, :, None, :, None, :, None] * b[None, :, None, :, None, :, None, :]
        return both.reshape(SPAN, SPAN, SPAN, SPAN)

    re = outer(real, real) - outer(imag, imag)
    im = outer(real, imag) + outer(imag, real)
    top = jnp.stack([re, -im], axis=2)
    bottom = jnp.stack([im, re], axis=2)
    return jnp.stack([top, bottom], axis=0)


def exchange(x, groups=None):
    return lax.all_to_all(
        x, AXES, split_axis=0, concat_axis=0, tiled=True, axis_index_groups=groups
    )


def swap_local(x, local):
    shaped = x.reshape(x.shape[0] // local, local, 2, local)
    return jnp.transpose(shaped, (0, 3, 2, 1)).reshape(x.shape)


def simple_per_device(rho, perm, superop):
    full = rho.shape[2]
    local = rho.shape[1]
    side = 2 * SPAN * SPAN
    table0 = relabel_table(perm[0], full)
    table1 = relabel_table(perm[1], full)
    kernel0 = jnp.transpose(pair_kernel(superop[0]), (1, 0, 2, 4, 3, 5)).reshape(side, side)
    kernel1 = jnp.transpose(pair_kernel(superop[1]), (2, 0, 1, 5, 3, 4)).reshape(side, side)

    x = rho.reshape(2 * local, full).T
    x = gather_rows(x, table0)
    x = exchange(x)
    x = swap_local(x, local)
    x = gather_turn(x, table0)
    x = apply_channel(x, kernel0)
    x = jnp.transpose(x, (2, 0, 1)).reshape(full, 2 * local)
    x = gather_rows(x, table1)
    x = exchange(x)
    x = swap_local(x, local)
    x = gather_turn(x, table1)
    x = apply_channel(x, kernel1)
    x = jnp.transpose(x, (2, 0, 1)).reshape(full, 2 * local)
    matrix = x.T.reshape(2, local, full)

    return matrix


def params():
    return pltpu.CompilerParams(vmem_limit_bytes=VMEM_LIMIT)


def cost(flops, nbytes):
    return pl.CostEstimate(flops=flops, bytes_accessed=nbytes, transcendentals=0)


def whole():
    return pl.BlockSpec(memory_space=pltpu.VMEM)


def scalars():
    return pl.BlockSpec(memory_space=pltpu.SMEM)


def two_parts(x):
    big = x.astype(jnp.bfloat16)
    return big, (x - big.astype(jnp.float32)).astype(jnp.bfloat16)


def reorder(order, x):
    big, small = two_parts(x)
    y = jnp.dot(order, small, preferred_element_type=jnp.float32)
    return y + jnp.dot(order, big, preferred_element_type=jnp.float32)


def copy_rows(idx_ref, first, step, count, parts, src_ref, dst_ref, base, whole_row=None, skip=0):
    pitch = parts if whole_row is None else whole_row
    near = [idx_ref[step * k] * pitch for k in range(8)]

    @pl.loop(0, count // 32)
    def _(block):
        start = block * 32
        for far in range(0, 32, 8):
            origin = idx_ref[first + step * (start + far)] * pitch + skip
            for k in range(8):
                src = pl.multiple_of(origin + near[k], parts)
                dst = pl.multiple_of((base + start + far + k) * parts, parts)
                dst_ref[pl.ds(dst, parts), :] = src_ref[pl.ds(src, parts), :]


def superop_body(by_row, s_ref, o_ref):
    at = lax.broadcasted_iota(jnp.int32, (SIDE, SPAN), 0)
    entry = lax.broadcasted_iota(jnp.int32, (SIDE, SPAN), 1)
    first, last_ = at // (2 * SPAN), at % SPAN
    row, col = (first, last_) if by_row else (last_, first)

    def spread(pair, values):
        mine = jnp.right_shift(row, 2 * pair) % 4 * 4 + jnp.right_shift(col, 2 * pair) % 4
        pick_ = jnp.where(mine == entry, 1.0, 0.0)
        rows = jnp.dot(
            pick_, values, precision=lax.Precision.HIGHEST, preferred_element_type=jnp.float32
        )
        return lax.dot_general(
            rows,
            pick_,
            (((1,), (1,)), ((), ())),
            precision=lax.Precision.HIGHEST,
            preferred_element_type=jnp.float32,
        )

    re0, im0 = spread(0, s_ref[0]), spread(0, s_ref[1])
    re1, im1 = spread(1, s_ref[0]), spread(1, s_ref[1])
    re = re1 * re0 - im1 * im0
    im = re1 * im0 + im1 * re0
    out_im = lax.broadcasted_iota(jnp.int32, (SIDE, SIDE), 0) // SPAN % 2
    in_im = lax.broadcasted_iota(jnp.int32, (SIDE, SIDE), 1) // SPAN % 2
    o_ref[...] = jnp.where(out_im == in_im, re, jnp.where(out_im == 1, im, -im))


def superop_matrix(layer_super, by_row):
    return pl.pallas_call(
        functools.partial(superop_body, by_row),
        out_shape=jax.ShapeDtypeStruct((SIDE, SIDE), jnp.float32),
        in_specs=[whole()],
        out_specs=whole(),
        compiler_params=params(),
        cost_estimate=cost(10**8, 10**6),
        name="superop",
    )(layer_super)


def turn_body(x_ref, o_ref):
    parts = x_ref.shape[0] // LANES
    cols = x_ref.shape[1]
    for k in range(parts):
        o_ref[pl.ds(k, cols, stride=parts), :] = x_ref[pl.ds(k * LANES, LANES), :].T


def turn_order_body(order_ref, x_ref, o_ref):
    parts = x_ref.shape[0] // LANES
    cols = x_ref.shape[1]
    half = parts // 2
    order = order_ref[...].astype(jnp.bfloat16)
    for part in range(2):
        x = reorder(order, x_ref[pl.ds(part * half * LANES, half * LANES), :])
        for k in range(half):
            o_ref[pl.ds(k * 2 + part, cols, stride=parts), :] = x[k * LANES : (k + 1) * LANES].T


def turn(x, order=None):
    height, full = x.shape
    parts = height // LANES
    cols = 512
    extra = [] if order is None else [order]
    return pl.pallas_call(
        turn_body if order is None else turn_order_body,
        out_shape=jax.ShapeDtypeStruct((full * parts, LANES), x.dtype),
        grid=(full // cols,),
        in_specs=[pl.BlockSpec(o.shape, lambda i: (0, 0)) for o in extra]
        + [pl.BlockSpec((height, cols), lambda i: (0, i))],
        out_specs=pl.BlockSpec((cols * parts, LANES), lambda i: (i, 0)),
        compiler_params=params(),
        cost_estimate=cost(10**8, 2 * x.size * 4),
        name="turn",
    )(*extra, x)


def pick_body(groups, share, devices, parts, idx_ref, x_ref, *outs):
    count = share // GROUPS
    targets = outs[0].shape[0]
    senders = x_ref.shape[0] // (parts * idx_ref.shape[0])
    start = pl.program_id(0) * targets

    @pl.loop(0, targets)
    def _(i):
        d = start + i
        skip = d // devices * parts
        for group, out in zip(groups, outs):
            first = d % devices * share + group * count
            copy_rows(idx_ref, first, 1, count, parts, x_ref, out.at[i], 0, senders * parts, skip)


def pick(xt, table, groups, devices, parts):
    full = table.shape[0]
    share = full // devices
    targets = devices * (xt.shape[0] // (full * parts))
    steps = 4
    rows = share // GROUPS * parts
    spec = pl.BlockSpec((targets // steps, rows, LANES), lambda i, s: (i, 0, 0))
    return pl.pallas_call(
        functools.partial(pick_body, groups, share, devices, parts),
        out_shape=[jax.ShapeDtypeStruct((targets, rows, LANES), xt.dtype)] * len(groups),
        grid_spec=pltpu.PrefetchScalarGridSpec(
            num_scalar_prefetch=1, grid=(steps,), in_specs=[whole()], out_specs=[spec] * len(groups)
        ),
        compiler_params=params(),
        cost_estimate=cost(10**8, 3 * xt.size * 4),
        name="pick",
    )(table, xt)


def mix(idx_ref, w_ref, g, xk, tmp):
    high = tmp.shape[0] // 2
    groups = LANES // SPAN

    @pl.loop(0, SPAN)
    def _(low):
        copy_rows(idx_ref, low, SPAN, high, 2, g, tmp, 0)
        for part in range(2):
            turned = tmp[pl.ds(part, high, stride=2), :].T
            at = pl.multiple_of(low * 2 * SPAN + part * SPAN, SPAN)
            xk[:, pl.ds(at, SPAN), :] = turned.reshape(groups, SPAN, high)

    w_big, w_small = two_parts(w_ref[...])

    @pl.loop(0, groups)
    def _(group):
        x_big, x_small = two_parts(xk[group])
        y = jnp.dot(w_big, x_small, preferred_element_type=jnp.float32)
        y += jnp.dot(w_small, x_big, preferred_element_type=jnp.float32)
        y += jnp.dot(w_big, x_big, preferred_element_type=jnp.float32)
        xk[group] = y


def middle_body(chunks, count, blocks, idx_ref, next_ref, w_ref, r_ref, *refs):
    *outs, g, xk, tmp = refs
    sources = r_ref.shape[0]
    parts = r_ref.shape[1] // (LANES * chunks)
    halves = parts // 2
    local = halves * LANES
    high = tmp.shape[0] // 2
    rows = next_ref.shape[0] // (outs[0].shape[0] * blocks)

    @pl.loop(0, chunks)
    def _(c):
        @pl.loop(0, sources)
        def _(s):
            for k in range(parts):
                part, half = k // halves, k % halves
                block = r_ref[s, pl.ds(c * (LANES * parts) + k, LANES, stride=parts), :]
                at = (s * local + half * LANES) * 2 + part
                g[pl.ds(at, LANES, stride=2), :] = block.T

        mix(idx_ref, w_ref, g, xk, tmp)

        @pl.loop(0, SPAN)
        def _(low):
            for part in range(2):
                at = pl.multiple_of(low * 2 * SPAN + part * SPAN, SPAN)
                block = xk[:, pl.ds(at, SPAN), :].reshape(LANES, high)
                g[pl.ds(low * high * 2 + part, high, stride=2), :] = block.T

        @pl.loop(0, outs[0].shape[0])
        def _(d):
            for b in range(blocks):
                out, base = (outs[0], (c * blocks + b) * rows) if count == 1 else (outs[b], c * rows)
                copy_rows(next_ref, (d * blocks + b) * rows, 1, rows, 2, g, out.at[d], base)


def middle(r, table, next_table, w, chunks, devices, blocks, split):
    full = table.shape[0]
    high = full // SPAN
    count = blocks if split else 1
    rows = next_table.shape[0] // (devices * blocks) * chunks * (blocks // count)
    message = jax.ShapeDtypeStruct((devices, 2 * rows, LANES), r.dtype)
    return pl.pallas_call(
        functools.partial(middle_body, chunks, count, blocks),
        out_shape=[message] * count,
        in_specs=[scalars(), scalars(), whole(), whole()],
        out_specs=[whole()] * count,
        scratch_shapes=[
            pltpu.VMEM((full * 2, LANES), r.dtype),
            pltpu.VMEM((LANES // SPAN, SIDE, high), r.dtype),
            pltpu.VMEM((high * 2, LANES), r.dtype),
        ],
        compiler_params=params(),
        cost_estimate=cost(2 * 3 * SIDE * r.size, 2 * r.size * 4),
        name="middle",
    )(table, next_table, w, r)


def last_body(chunks, which, blocks, paired, idx_ref, mine_ref, w_ref, *refs):
    if paired:
        order_ref, *refs = refs
    rs = refs[:GROUPS]
    o_ref, t_ref, g, xk, tmp = refs[-5:]
    full = idx_ref.shape[0]
    high = tmp.shape[0] // 2
    step = pl.program_id(0)
    sources = rs[0].shape[0] // (2 if paired else 1)
    rows = LANES // (2 if paired else 1)
    share = full // sources

    @pl.when(step == 0)
    def _():
        if paired:
            order = order_ref[...].astype(jnp.bfloat16)

        @pl.loop(0, sources)
        def _(s):
            for a, r_ref in enumerate(rs):
                there = blocks if r_ref.shape[1] == 2 * rows * chunks * blocks else 1
                for c in range(chunks):
                    for part in range(2):
                        base = (c * there + (which if there > 1 else 0)) * rows * 2 + part
                        at = pl.ds(base, rows, stride=2)
                        if paired:
                            block = jnp.concatenate([r_ref[s, at, :], r_ref[s + sources, at, :]])
                            block = reorder(order, block)
                        else:
                            block = r_ref[s, at, :]
                        to = (s * share + (a * chunks + c) * LANES) * 2 + part
                        g[pl.ds(to, LANES, stride=2), :] = block.T

        mix(idx_ref, w_ref, g, xk, tmp)

        @pl.loop(0, SPAN)
        def _(low):
            for part in range(2):
                at = pl.multiple_of(low * 2 * SPAN + part * SPAN, SPAN)
                block = xk[:, pl.ds(at, SPAN), :].reshape(LANES, high)
                g[pl.ds(part * full + low, high, stride=SPAN), :] = block.T

    cols = o_ref.shape[2]
    for part in range(2):
        at = pl.multiple_of(part * full + step * cols, LANES)
        o_ref[part] = g[pl.ds(at, cols), :].T

    diagonal = mine_ref[0] + which * LANES

    @pl.when(step == diagonal // cols)
    def _():
        square = o_ref[0, :, pl.ds(pl.multiple_of(diagonal % cols, LANES), LANES)]
        row = lax.broadcasted_iota(jnp.int32, square.shape, 0)
        col = lax.broadcasted_iota(jnp.int32, square.shape, 1)
        mine = jnp.sum(jnp.where(row == col, square, 0.0), axis=0, keepdims=True)
        t_ref[...] = mine + refs[GROUPS][...] if which else mine


def last(rs, table, mine, w, order, chunks, which, blocks, before):
    full = table.shape[0]
    high = full // SPAN
    cols = 1024
    orders = [] if order is None else [order]
    ins = [table, mine, w, *orders, *rs]
    return pl.pallas_call(
        functools.partial(last_body, chunks, which, blocks, order is not None),
        out_shape=(
            jax.ShapeDtypeStruct((2, blocks * LANES, full), rs[0].dtype),
            jax.ShapeDtypeStruct((1, LANES), rs[0].dtype),
        ),
        grid=(full // cols,),
        in_specs=[scalars()] * 2
        + [whole()] * (len(ins) - 2)
        + [whole(), pl.BlockSpec(memory_space=pl.ANY)][: len(before)],
        out_specs=(
            pl.BlockSpec((2, LANES, cols), lambda i: (0, which, i)),
            pl.BlockSpec((1, LANES), lambda i: (0, 0)),
        ),
        scratch_shapes=[
            pltpu.VMEM((full * 2, LANES), rs[0].dtype),
            pltpu.VMEM((LANES // SPAN, SIDE, high), rs[0].dtype),
            pltpu.VMEM((high * 2, LANES), rs[0].dtype),
        ],
        input_output_aliases={len(ins) + 1: 0} if before else {},
        compiler_params=params(),
        cost_estimate=cost(2 * 3 * SIDE * full * 2 * LANES, 4 * full * 2 * LANES * 4),
        name="last",
    )(*ins, *before[::-1])


def sum_over_devices(value, devices):
    return jnp.sum(exchange(jnp.broadcast_to(value, (devices, value.shape[1]))))


def after(x, *done):
    return lax.optimization_barrier((x, *done))[0]


def bit_in(x, at):
    low = jnp.left_shift(1, at) - 1
    return jnp.left_shift(x - (x & low), 1) + (x & low)


def bit_out(x, at):
    low = jnp.left_shift(1, at) - 1
    return jnp.left_shift(jnp.right_shift(x, at + 1), at) + (x & low)


def spread(q, count):
    return q % SPAN * (count // SPAN) + q // SPAN


def run_plan(plan, rho, perm, superop, marks, devices):
    full = rho.shape[2]
    local = full // devices
    blocks = local // LANES
    top = full // 2
    half = devices // 2
    halves = [list(range(half)), list(range(half, devices))]
    table0 = relabel_table(perm[0], full)
    kept, place, final, source = (marks[k] for k in range(4))
    x = rho.reshape(2 * local, full)
    q = jnp.arange(top, dtype=jnp.int32)
    first_groups = second_groups = order = None

    if plan == "full":
        share, parts, chunks = devices, 2 * blocks, 1
        xt = turn(x)
        rows0 = table0
        rows1 = spread(relabel_table(perm[1], full), full)
        targets = devices
    else:
        share, chunks = half, 2
        if plan == "send_keep":
            parts = 2
            at = jnp.arange(local, dtype=jnp.int32)
            new = bit_out(at, source) + (jnp.right_shift(at, source) & 1) * (local // 2)
            xt = turn(x, jnp.where(at[:, None] == new[None, :], 1.0, 0.0))
            old = relabel(bit_in(q, final), perm[0])
            rows0 = old // local * (local // 2) + bit_out(old % local, source)
            stays = final
        else:
            parts = 2 * blocks
            first_groups = halves
            xt = turn(x)
            rows0 = relabel(bit_in(q, kept), perm[0])
            stays = kept
        if plan == "keep_send":
            targets = devices
            few = LANES // 2
            row = q // few * LANES + bit_in(q % few, place)
            at = jnp.arange(LANES, dtype=jnp.int32)
            from_two = bit_in(at % few, place) + jnp.left_shift(at // few, place)
            order = jnp.where(at[:, None] == from_two[None, :], 1.0, 0.0)
        else:
            targets = half
            second_groups = halves
            row = q
        rows1 = spread(bit_out(relabel(row, perm[1]), stays), top)

    table1 = relabel_table(perm[1], full)
    got = []
    if first_groups is None:
        sent = [pick(xt, table0, (a,), share, parts)[0] for a in range(GROUPS)]
        got.append(exchange(sent[0]))
    else:
        sent = pick(xt, table0, tuple(range(GROUPS)), share, parts)
        got.append(exchange(after(*sent), first_groups))
    for message in sent[1:]:
        got.append(exchange(after(message, got[-1]), first_groups))
    kernel0 = superop_matrix(superop[0], True)
    kernel1 = superop_matrix(superop[1], False)
    done = got[-1]
    parts_of = [[] for _ in range(blocks)]
    for a in range(GROUPS):
        split = a == GROUPS - 1
        messages = middle(got[a], rows0, rows1, kernel0, chunks, targets, blocks, split)
        arrived = []
        for message in messages:
            done = exchange(after(message, done), second_groups)
            arrived.append(done)
        for b in range(blocks):
            parts_of[b].append(arrived[b] if split else arrived[0])
    done = ()
    mine = jnp.reshape(lax.axis_index(AXES).astype(jnp.int32) * local, (1,))
    for b in range(blocks):
        done = last(parts_of[b], table1, mine, kernel1, order, chunks, b, blocks, done)
    return done


def mark_bits(perm):
    qubits = jnp.arange(perm.shape[1], dtype=jnp.int32)
    kept = jnp.sum(jnp.where(perm[0] == qubits[-1], qubits, 0))
    place = jnp.sum(jnp.where(perm[1] == kept, qubits, 0))
    final = perm[1][-1]
    source = jnp.sum(jnp.where(qubits == final, perm[0], 0))
    return jnp.stack([kept, place, final, source])


def choose_plan(marks, local, top_bit):
    low_bits = (SPAN - 1).bit_length()
    kept, place, final, source = (marks[k] for k in range(4))
    plain = kept >= low_bits
    keep_send = plain & (place < LANES.bit_length() - 1)
    keep_keep = plain & (place == top_bit)
    send_keep = (final >= low_bits) & (source < local.bit_length() - 1)
    return jnp.where(keep_send, 3, jnp.where(keep_keep, 0, jnp.where(send_keep, 1, 2)))


def chunked_per_device(rho, perm, superop):
    full = rho.shape[2]
    local = rho.shape[1]
    devices = full // local
    plans = ("keep_keep", "send_keep", "full", "keep_send")
    runs = [functools.partial(run_plan, plan, devices=devices) for plan in plans]
    marks = mark_bits(perm)
    plan = choose_plan(marks, local, perm.shape[1] - 1)
    return lax.switch(plan, runs, rho, perm, superop, marks)


def per_device(rho, perm, superop):
    full = rho.shape[2]
    local = rho.shape[1]
    if local == GROUPS * LANES:
        matrix, diagonal = chunked_per_device(rho, perm, superop)
    else:
        matrix = simple_per_device(rho, perm, superop)
        position = lax.axis_index(AXES)
        block = lax.dynamic_slice_in_dim(matrix[0], position * local, local, 1)
        diagonal = jnp.broadcast_to(jnp.trace(block) / LANES, (1, LANES))
    return (matrix, sum_over_devices(diagonal, full // local) / full)


def solution(mesh):
    assert PAIRS == 2
    placed = (P(None, AXES, None), P(), P())
    return jax.shard_map(
        per_device,
        mesh=mesh,
        in_specs=placed,
        out_specs=(P(None, AXES, None), P()),
        check_vma=False,
    )
```
